32 devices in a mesh: dp: 4 (over z), bal: 4 (over x, core), tensor: 2 (over y).
Axes of the slice: x: 2, y: 2, z: 4, core: 2. Of those that a mesh axis runs over, the one named last changes fastest.
Arguments:
- tiles: bfloat16 [4, 4, 16, 1280, 128], P('dp', 'bal', None, 'tensor'), may hold values from -6 to 6
- tile_counts: int32 [4, 4], P('dp'), may hold values from 1 to 16, 32 in all within a row
- doc_order: int32 [4, 4], P('dp'), may hold values from 0 to 3, each once within a row
- qkv_weight: bfloat16 [3, 1280, 1280], P(None, 'dp', 'tensor'), may hold values from -6 to 6
- out_weight: bfloat16 [1280, 1280], P('dp', 'tensor'), may hold values from -0.625 to 0.625
Outputs:
- encoded: bfloat16 [4, 32, 1280, 128], P('dp', 'bal', 'tensor')
The draws below stay inside these ranges and needn't reach their ends.
Inputs may be any that keep to these rules, and one draw needn't show every extreme that they name: `tile_counts`: each row sums to 32, and in every row some document has exactly 16 tiles. `doc_order`: each row names every document once.
All inputs are finite; a program needn't handle non-finite values.
Results may differ from the reference program's by a relative error of at most 0.012.
Values may be sent and summed in bfloat16 or wider, within the bound.
A program may use at most 64 MiB of HBM per device.

```python
import math
import jax
import jax.numpy as jnp
import numpy as np
from jax import lax

D = 1280
HEADS = 16
HDIM = 80
PATCH = 128
TILE_MAX = 16
CAP = 8
DOCS = 4
POSITIONS = 32
HEAD_GROUPS = 2
N_DP = 4


def draw_qkv_weight(key, part):
    standard = jnp.clip(jax.random.normal(key, (3, D, D), jnp.float32), -6.0, 6.0) * D ** (-0.5)
    return standard.astype(jnp.bfloat16)


def shard_levels(key, extent, pieces, smallest, high):
    def one(dim, shards_of):
        heights = jax.random.uniform(jax.random.fold_in(jax.random.fold_in(key, 6), dim), (shards_of,), jnp.float32, smallest / len(pieces), high / len(pieces))
        return jnp.repeat(jnp.exp(heights), extent[dim] // shards_of).reshape((-1,) + (1,) * (len(extent) - dim - 1))

    factor_of = one(*pieces[0])
    for cut in pieces[1:]:
        factor_of = factor_of * one(*cut)
    return factor_of


def length_profile(number_of, total, most, skew):
    portions = [(1 << 20) // math.isqrt(grade ** skew) + 1 for grade in range(2, number_of + 1)]
    surplus, given = total - most - (number_of - 1), [1] * (number_of - 1)
    while surplus > 0:
        candidates = [i for i in range(number_of - 1) if given[i] < most]
        mass, budget = sum([portions[i] for i in candidates]), surplus
        for i in candidates:
            more = min(most - given[i], max(1, budget * portions[i] // mass), surplus)
            given[i] = given[i] + more
            surplus = surplus - more
    return np.array([most] + given)


def ragged(own_key, amount, total, reach, skew):
    if amount == 2:
        one = jax.random.randint(own_key, (), max(1, total - reach), min(reach, total - 1) + 1)
        return jnp.stack([one, total - one])
    sizes = jnp.asarray(length_profile(amount, total, reach, skew), jnp.int32)
    couples = (amount - 1) // 2
    giver, sink = sizes[1:1 + 2 * couples:2], sizes[2:2 + 2 * couples:2]
    margin = jnp.minimum(giver - 1, reach - sink)
    shifted = jax.random.randint(jax.random.fold_in(own_key, 1), (couples,), 0, 1 << 20) % (margin + 1)
    sizes = sizes.at[1:1 + 2 * couples:2].set(giver - shifted).at[2:2 + 2 * couples:2].set(sink + shifted)
    return sizes[jax.random.permutation(jax.random.fold_in(own_key, 2), amount)]


def normal_values(rng, extent, deviation, most, split=(), kind=jnp.bfloat16):
    array = deviation * jax.random.normal(rng, extent, jnp.float32)
    if split:
        array = array * shard_levels(rng, extent, split, -0.22, 0.18)
    return jnp.clip(array, -most, most).astype(kind)


def setup_inputs(seed: int = 0) -> dict:
    key_list = jax.random.split(jax.random.key(seed), 6)
    tiles = normal_values(key_list[0], (N_DP, DOCS, TILE_MAX, D, PATCH), 1.0, 6.0, ((0, 4), (1, 4), (3, 2)))
    tile_counts = jax.vmap(lambda own: ragged(own, DOCS, POSITIONS, TILE_MAX, 2))(jax.random.split(key_list[1], N_DP)).reshape((N_DP, DOCS)).astype(jnp.int32)
    doc_order = jax.vmap(lambda own: jax.random.permutation(own, DOCS))(jax.random.split(key_list[2], N_DP)).reshape((N_DP, DOCS)).astype(jnp.int32)
    qkv_weight = draw_qkv_weight(jax.random.fold_in(key_list[5], 71), 0)
    out_weight = normal_values(key_list[4], (D, D), HDIM ** -0.5, 0.625, ((0, 4), (1, 2)))
    return {"tiles": tiles, "tile_counts": tile_counts, "doc_order": doc_order, "qkv_weight": qkv_weight, "out_weight": out_weight}


EPSILON = 1e-06

def normalize(tile_rows):
    values = tile_rows.astype(jnp.float32)
    center = values - lax.optimization_barrier(jnp.mean(values, axis=-1, keepdims=True))
    spread = lax.optimization_barrier(jnp.mean(center * center, axis=-1, keepdims=True))
    return (center * lax.rsqrt(spread + EPSILON)).astype(jnp.bfloat16)

def encode(tile_block, qkv_weight, out_weight):
    tile_total = tile_block.shape[0]
    row_count = tile_total * PATCH
    normed = normalize(tile_block).reshape(row_count, D)
    flat_weight = jnp.transpose(qkv_weight, (1, 0, 2)).reshape(D, 3 * D)
    projected = jnp.dot(normed, flat_weight, preferred_element_type=jnp.float32).astype(jnp.bfloat16)
    projected = projected.reshape(tile_total, PATCH, 3, HEADS, HDIM)
    query = projected[:, :, 0].astype(jnp.float32)
    key_rows = projected[:, :, 1].astype(jnp.float32)
    value_rows = projected[:, :, 2].astype(jnp.float32)
    scores = jnp.einsum('rqhe,rkhe->rhqk', query, key_rows) * HDIM ** (-0.5)
    probs = jax.nn.softmax(scores, axis=-1).astype(jnp.bfloat16)
    context = jnp.einsum('rhqk,rkhe->rqhe', probs.astype(jnp.float32), value_rows).astype(jnp.bfloat16)
    context = context.reshape(row_count, D)
    group_width = D // HEAD_GROUPS
    running = tile_block.astype(jnp.float32).reshape(row_count, D)
    for group in range(HEAD_GROUPS):
        low = group * group_width
        partial_value = jnp.dot(context[:, low:low + group_width], out_weight[:, low:low + group_width].T, preferred_element_type=jnp.float32)
        rounded = lax.optimization_barrier(partial_value.astype(jnp.bfloat16))
        running = running + rounded.astype(jnp.float32)
    return running.astype(jnp.bfloat16).reshape(tile_total, PATCH, D)

def reference(tiles, tile_counts, doc_order, qkv_weight, out_weight):
    doc_ids = jnp.arange(DOCS, dtype=jnp.int32)

    def group_index(counts, ordering):
        position = lax.optimization_barrier(jnp.sum(jnp.where(ordering[None, :] == doc_ids[:, None], doc_ids[None, :], 0), axis=1))
        starts = lax.optimization_barrier(jnp.sum(jnp.where(position[None, :] < position[:, None], counts[None, :], 0), axis=1))
        packed = jnp.arange(POSITIONS, dtype=jnp.int32)
        inside = (starts[None, :] <= packed[:, None]) & (packed[:, None] < (starts + counts)[None, :])
        source = lax.optimization_barrier(jnp.sum(jnp.where(inside, doc_ids[None, :], 0), axis=1))
        offset = packed - lax.optimization_barrier(jnp.sum(jnp.where(inside, starts[None, :], 0), axis=1))
        return (source * TILE_MAX + offset).astype(jnp.int32)
    flat_index = jax.vmap(group_index)(tile_counts, doc_order)
    group_base = (jnp.arange(N_DP, dtype=jnp.int32) * (DOCS * TILE_MAX)).astype(jnp.int32)
    flat_index = (flat_index + group_base[:, None]).astype(jnp.int32)
    flat_tiles = jnp.swapaxes(tiles, 3, 4).reshape(N_DP * DOCS * TILE_MAX, PATCH, D)
    packed_tiles = jnp.take(flat_tiles, flat_index.reshape(-1), axis=0)
    blocks = packed_tiles.reshape(N_DP * POSITIONS // CAP, CAP, PATCH, D)
    encoded = lax.map(lambda tile_block: encode(tile_block, qkv_weight, out_weight), blocks)
    return jnp.swapaxes(encoded.reshape(N_DP, POSITIONS, PATCH, D), 2, 3)
```

```python
import functools

import jax
import jax.numpy as jnp
from jax import lax
from jax.experimental import pallas as pl
from jax.experimental.pallas import tpu as pltpu
from jax.sharding import PartitionSpec as P

HDIM = 80
CAP = 8
LANES = 128
GROUP = 4
EPSILON = 1e-06
LOG2E = 1.4426950408889634
MESH = pl.DeviceIdType.MESH


def flip(index, bit):
    return index + bit - 2 * bit * ((index // bit) % 2)


def bits_of(size):
    bits = []
    while 1 << len(bits) < size:
        bits.append(1 << len(bits))
    return bits


def column_groups(slices):
    width = LANES if slices % LANES == 0 else slices
    return width, slices // width


def pieces_of(slices):
    half = slices // 2
    first = [(0, 0, half), (0, half, half)] if half % 16 == 0 else [(0, 0, slices)]
    return first + [(i, 0, slices) for i in range(1, CAP)]


def remote(src, dst, send, recv, **device):
    return pltpu.make_async_remote_copy(
        src_ref=src, dst_ref=dst, send_sem=send, recv_sem=recv, device_id=device, device_id_type=MESH
    )


def encode_kernel(sizes, *refs):
    nd, nb, nt = sizes
    bits = bits_of(nb)
    ns = len(bits)
    counts, order, tiles_in, wq_in, wo_in, out = refs[:6]
    sends, recvs = refs[6 : 6 + ns], refs[6 + ns : 6 + 2 * ns]
    tiles, gath, wq, wt, wo_own, wo, normed, qkv, ctx, own = refs[6 + 2 * ns : 16 + 2 * ns]
    sems = refs[16 + 2 * ns :]
    t_send, t_recv, y_send, y_recv, c_send, c_recv = sems[:6]
    l_send, l_recv, h_send, h_recv = sems[6:10]
    x_send, x_recv, w_send, w_recv, d_send, d_recv, i_sem = sems[10:]
    z, b, t = lax.axis_index("dp"), lax.axis_index("bal"), lax.axis_index("tensor")
    _, slices, patches = tiles.shape
    width, groups = column_groups(slices)
    pieces = pieces_of(slices)
    per = nd // nt
    features = nt * slices
    kinds = wq.shape[0]
    blocks = CAP // GROUP

    load_tiles = pltpu.make_async_copy(tiles_in, tiles, i_sem.at[0])
    load_q = pltpu.make_async_copy(wq_in, wq.at[:, z], i_sem.at[1])
    load_o = pltpu.make_async_copy(wo_in, wo_own, i_sem.at[2])
    load_tiles.start()
    load_q.start()
    load_o.start()

    barrier = pltpu.get_barrier_semaphore()
    for m in bits:
        pl.semaphore_signal(barrier, inc=1, device_id={"bal": flip(b, m)}, device_id_type=MESH)
    for j in range(1, nt):
        pl.semaphore_signal(barrier, inc=1, device_id={"tensor": (t + j) % nt}, device_id_type=MESH)

    def greet(j, carry):
        pl.semaphore_signal(barrier, inc=1, device_id={"dp": (z + j) % nd}, device_id_type=MESH)
        return carry

    lax.fori_loop(1, nd, greet, 0)

    docs = order.shape[1]
    placed = [order[0, p] for p in range(docs)]
    edges = [jnp.int32(0)]
    for doc in placed:
        edges.append(edges[-1] + counts[0, doc])
    own_start = jnp.int32(0)
    for p in range(docs):
        own_start = own_start + jnp.where(placed[p] == b, edges[p], 0)

    def slot_of(s, r):
        return r >> (s + 1)

    def current(s, r, i, rows):
        block = b
        for m in bits:
            if r & m:
                block = flip(block, m)
        packed = block * CAP + i
        owner = jnp.int32(0)
        for p in range(docs):
            inside = (edges[p] <= packed) & (packed < edges[p + 1])
            owner = owner + jnp.where(inside, placed[p], 0)
        value = tiles[jnp.clip(packed - own_start, 0, tiles.shape[0] - 1), rows]
        for q in range(s):
            apart = (owner // bits[q]) % 2 != (b // bits[q]) % 2
            value = lax.select(apart, recvs[q][slot_of(q, r), i, rows], value)
        return value

    def tile_copy(s, slot, p):
        i, start, count = pieces[p]
        rows = pl.ds(start, count)
        return remote(
            sends[s].at[slot, i, rows],
            recvs[s].at[slot, i, rows],
            t_send.at[s, slot, p],
            t_recv.at[s, slot, p],
            bal=flip(b, bits[s]),
        )

    def wait_for(s, r, p):
        for q in range(s):
            tile_copy(q, slot_of(q, r), p).wait_recv()

    def wanted(s):
        m = bits[s]
        return [r for r in reversed(range(nb)) if r & (m - 1) == 0 and r & m]

    load_tiles.wait()
    for r in wanted(0):
        slot = slot_of(0, r - 1)

        def fill(i, carry, r=r, slot=slot):
            sends[0][slot, i] = current(0, r, i, slice(None))
            return carry

        lax.fori_loop(0, CAP, fill, 0)

    load_o.wait()
    load_q.wait()
    keeper = z // per
    place = z % per

    @pl.when(keeper == t)
    def _():
        wo[t, place, b] = wo_own[b]

    pl.semaphore_wait(barrier, ns + nt - 1 + nd - 1)

    for r in wanted(0):
        for p in range(len(pieces)):
            tile_copy(0, slot_of(0, r - 1), p).start()

    part_count = wq.shape[2]
    part = b % part_count

    def held(src, k):
        return wq.at[:, jnp.clip(src, 0, nd - 1), part, :, pl.ds(k * width, width)]

    def line(way, s, k):
        step = 1 - 2 * way
        src = z - step * s
        there = z + step
        valid = (src >= 0) & (src < nd) & (there >= 0) & (there < nd)
        at = held(src, k)
        copy = remote(
            at, at, l_send.at[way, s, k], l_recv.at[way, s, k], dp=jnp.clip(there, 0, nd - 1)
        )
        return valid, copy

    def arrival(way, s, k):
        step = 1 - 2 * way
        src = z - step * (s + 1)
        valid = (src >= 0) & (src < nd)
        at = held(src, k)
        here = remote(
            at, at, l_send.at[way, s, k], l_recv.at[way, s, k], dp=jnp.clip(z + step, 0, nd - 1)
        )
        half = remote(at, at, h_send.at[way, s, k], h_recv.at[way, s, k], bal=flip(b, 1))
        return valid, here, half

    for k in range(groups):
        for way in range(2):
            valid, copy = line(way, 0, k)
            pl.when(valid)(copy.start)

    def hop(s, k):
        for way in range(2):
            valid, here, half = arrival(way, s, k)
            further, copy = line(way, s + 1, k)

            @pl.when(valid)
            def _(here=here, half=half, further=further, copy=copy):
                here.wait_recv()
                pl.when(further)(copy.start)
                if part_count > 1:
                    half.start()

    def halves(s, k):
        for way in range(2):
            valid, _, half = arrival(way, s, k)
            if part_count > 1:
                pl.when(valid)(half.wait_recv)

    def cross(source, target):
        return remote(
            wo_own.at[b], wo.at[source, place, b], x_send.at[0], x_recv.at[source], tensor=target
        )

    @pl.when(keeper != t)
    def _():
        cross(t, keeper).start()

    def spread(j):
        at = wo.at[:, place, b]
        return remote(at, at, w_send.at[j], w_recv.at[place], dp=(z + j) % nd)

    def spread_out():
        @pl.when(keeper == t)
        def _():
            for j in range(1, nt):
                cross((t + j) % nt, t).wait_recv()

            def start(j, carry):
                spread(j).start()
                return carry

            lax.fori_loop(1, nd, start, 0)

    def doubled(q, s, e):
        at = b
        for bit in range(s):
            if (e >> bit) & 1:
                at = flip(at, bits[ns - 1 - bit])
        rows = wo.at[:, q, at]
        index = (1 << s) - 1 + e
        return remote(
            rows, rows, d_send.at[q, index], d_recv.at[q, index], bal=flip(b, bits[ns - 1 - s])
        )

    def gathered(q):
        at = wo.at[:, q, b]
        return remote(at, at, w_send.at[0], w_recv.at[q], dp=(z + 1) % nd)

    def finish(s):
        def further(q, carry):
            if s == 0:
                pl.when(t * per + q != z)(gathered(q).wait_recv)
            else:
                for e in range(1 << (s - 1)):
                    doubled(q, s - 1, e).wait_recv()
            if s < ns:
                for e in range(1 << s):
                    doubled(q, s, e).start()
            return carry

        lax.fori_loop(0, per, further, 0)

    for s in range(1, ns):
        for r in wanted(s):
            slot = slot_of(s, r - bits[s])
            for p, (i, start, count) in enumerate(pieces):
                wait_for(s, r, p)
                rows = pl.ds(start, count)
                sends[s][slot, i, rows] = current(s, r, i, rows)
                tile_copy(s, slot, p).start()

    def y_copy(p, j):
        i, start, count = pieces[p]
        at = gath.at[i, pl.ds(pl.multiple_of(t * slices + start, 16), count), :]
        return remote(at, at, y_send.at[p, j], y_recv.at[p, j], tensor=(t + j) % nt)

    def normalize(i):
        for p, piece in enumerate(pieces):
            if piece[0] == i:
                for j in range(1, nt):
                    y_copy(p, j).wait_recv()
        values = gath[i].astype(jnp.float32)
        center = values - jnp.mean(values, axis=0, keepdims=True)
        spread_of = jnp.mean(center * center, axis=0, keepdims=True)
        normed[:, i * patches : (i + 1) * patches] = (
            center * lax.rsqrt(spread_of + EPSILON)
        ).astype(normed.dtype)

    early = min(2, nd - 1)
    forwards = [(s, k) for s in range(early) for k in range(groups)]
    slots = [1, 1, 2, 2, 3, 4, 5, 5, 6, 7]
    after = {}
    for n, pair in enumerate(forwards):
        after.setdefault(slots[n] if len(forwards) == len(slots) else CAP - 1, []).append(pair)
    for p, (i, start, count) in enumerate(pieces):
        wait_for(ns, 0, p)
        rows = pl.ds(start, count)
        gath[i, pl.ds(pl.multiple_of(t * slices + start, 16), count), :] = current(ns, 0, i, rows)
        for j in range(1, nt):
            y_copy(p, j).start()
        if start + count == slices:
            for s, k in after.get(i, []):
                hop(s, k)
            if i == 5:
                spread_out()
            if i >= 2:
                normalize(i - 2)

    def rest(k):
        def one(s, carry):
            hop(s, k)
            return carry

        lax.fori_loop(early, nd - 1, one, 0)

    def ready(k):
        def one(s, carry):
            halves(s, k)
            return carry

        lax.fori_loop(0, nd - 1, one, 0)
        for kind in range(kinds):
            block = wq[kind, :, :, :, k * width : (k + 1) * width].reshape(features, width)
            wt[kind * width : (kind + 1) * width, :] = block.T

    def heads_of(k):
        return [h for h in range(slices // HDIM) if k * width < (h + 1) * HDIM <= (k + 1) * width]

    def c_copy(k, g, j):
        first, number = heads_of(k)[0], len(heads_of(k))
        at = ctx.at[
            pl.ds(pl.multiple_of(t * slices + first * HDIM, 16), number * HDIM),
            pl.ds(pl.multiple_of(g * GROUP * patches, patches), GROUP * patches),
        ]
        return remote(at, at, c_send.at[k, g, j], c_recv.at[k, g, j], tensor=(t + j) % nt)

    def columns(i, number):
        return pl.ds(pl.multiple_of(i * patches, patches), number * patches)

    scale = HDIM ** (-0.5) * LOG2E

    def encode(k, g):
        for n in range(0, GROUP, 2):
            cols = columns(g * GROUP + n, 2)
            result = jnp.dot(wt[...], normed[:, cols], preferred_element_type=jnp.float32)
            for kind in range(kinds):
                qkv[kind, k * width : (k + 1) * width, cols] = result[
                    kind * width : (kind + 1) * width
                ].astype(qkv.dtype)
        for n in range(GROUP):
            cols = columns(g * GROUP + n, 1)
            for h in heads_of(k):
                span = slice(h * HDIM, (h + 1) * HDIM)
                scores = lax.dot_general(
                    qkv[1, span, cols], qkv[0, span, cols], (((0,), (0,)), ((), ())),
                    preferred_element_type=jnp.float32,
                )
                powers = jnp.exp2((scores - jnp.max(scores, axis=0, keepdims=True)) * scale)
                total = jnp.sum(powers, axis=0, keepdims=True)
                value = jnp.dot(
                    qkv[2, span, cols], powers.astype(qkv.dtype), preferred_element_type=jnp.float32
                )
                ctx[pl.ds(pl.multiple_of(t * slices + h * HDIM, 16), HDIM), cols] = (
                    value * (1.0 / total)
                ).astype(ctx.dtype)
        for j in range(1, nt):
            c_copy(k, g, j).start()

    rest(0)
    ready(0)
    encode(0, 0)
    if groups > 1:
        rest(1)
    for i in range(CAP - 2, CAP):
        normalize(i)

    def others(k, low):
        def one(g, carry):
            encode(k, g)
            return carry

        lax.fori_loop(low, blocks, one, 0)

    others(0, 1)
    for k in range(1, groups):
        ready(k)
        others(k, 0)
        if k + 1 < groups:
            rest(k + 1)
        if k <= ns:
            finish(k - 1)
    for s in range(min(groups - 1, ns), ns + 1):
        finish(s)

    def partial(source, cols):
        weight = wo[source].reshape(slices, slices)
        block = ctx[pl.ds(pl.multiple_of(source * slices, 16), slices), cols]
        return jnp.dot(weight, block, preferred_element_type=jnp.float32).astype(own.dtype)

    def mine(n, carry):
        own[:, columns(2 * n, 2)] = partial(t, columns(2 * n, 2))
        return carry

    lax.fori_loop(0, CAP // 2, mine, 0)

    def close(g, carry):
        for k in range(groups):
            for j in range(1, nt):
                c_copy(k, g, j).wait_recv()
        for n in range(0, GROUP, 2):
            i = g * GROUP + n
            total = own[:, columns(i, 2)].astype(jnp.float32)
            for j in range(1, nt):
                total = total + partial((t + j) % nt, columns(i, 2)).astype(jnp.float32)
            for e in range(2):
                source = gath[i + e, pl.ds(pl.multiple_of(t * slices, 16), slices), :]
                out[i + e] = (
                    source.astype(jnp.float32) + total[:, e * patches : (e + 1) * patches]
                ).astype(out.dtype)
        return carry

    lax.fori_loop(0, blocks, close, 0)

    for p in range(len(pieces)):
        for j in range(1, nt):
            y_copy(p, j).wait_send()
        for s in range(ns):
            for slot in range(nb >> (s + 1)):
                tile_copy(s, slot, p).wait_send()
    for k in range(groups):
        for j in range(1, nt):
            for g in range(blocks):
                c_copy(k, g, j).wait_send()

    @pl.when(keeper != t)
    def _():
        cross(t, keeper).wait_send()

    @pl.when(keeper == t)
    def _():
        def drain(j, carry):
            spread(j).wait_send()
            return carry

        lax.fori_loop(1, nd, drain, 0)

    def drain_doubled(q, carry):
        for s in range(ns):
            for e in range(1 << s):
                doubled(q, s, e).wait_send()
        return carry

    lax.fori_loop(0, per, drain_doubled, 0)

    def drain_line(s, carry):
        for k in range(groups):
            for way in range(2):
                valid, copy = line(way, s, k)
                pl.when(valid)(copy.wait_send)
                valid, _, half = arrival(way, s, k)
                if part_count > 1:
                    pl.when(valid)(half.wait_send)
        return carry

    lax.fori_loop(0, nd - 1, drain_line, 0)


def encode_all(counts, ordering, tiles, qkv_weight, out_weight):
    nd, nb, nt = (lax.axis_size(name) for name in ("dp", "bal", "tensor"))
    ns = len(bits_of(nb))
    slots, slices, patches = tiles.shape
    kinds, rows, columns = qkv_weight.shape
    width, groups = column_groups(columns)
    pieces = len(pieces_of(slices))
    per = nd // nt
    wq = qkv_weight.reshape(kinds, min(nb, 2), -1, columns)
    wo = out_weight.reshape(nb, -1, columns)
    dtype = tiles.dtype
    vmem = pl.BlockSpec(memory_space=pltpu.VMEM)
    hbm = pl.BlockSpec(memory_space=pltpu.HBM)
    dma = pltpu.SemaphoreType.DMA
    blocks = CAP // GROUP

    def space(*shape):
        return pltpu.VMEM(shape, dtype)

    buffers = [space(nb >> (s + 1), CAP, slices, patches) for s in range(ns)]
    return pl.pallas_call(
        functools.partial(encode_kernel, (nd, nb, nt)),
        out_shape=jax.ShapeDtypeStruct((CAP, slices, patches), dtype),
        in_specs=[pl.BlockSpec(memory_space=pltpu.SMEM)] * 2 + [hbm] * 3,
        out_specs=vmem,
        scratch_shapes=buffers
        + buffers
        + [
            space(slots, slices, patches),
            space(CAP, nt * slices, patches),
            space(kinds, nd, *wq.shape[1:]),
            space(kinds * width, nt * slices),
            space(*wo.shape),
            space(nt, per, *wo.shape),
            space(nt * slices, CAP * patches),
            space(kinds, columns, CAP * patches),
            space(nt * slices, CAP * patches),
            space(slices, CAP * patches),
        ]
        + [dma((ns, max(nb // 2, 1), pieces))] * 2
        + [dma((pieces, nt))] * 2
        + [dma((groups, blocks, nt))] * 2
        + [dma((2, nd, groups))] * 4
        + [dma((1,)), dma((nt,)), dma((nd,)), dma((per,))]
        + [dma((per, nb))] * 2
        + [dma((3,))],
        compiler_params=pltpu.CompilerParams(
            collective_id=0, has_side_effects=True, vmem_limit_bytes=44 * 1024 * 1024
        ),
        name="encode_all",
    )(counts, ordering, tiles, wq, wo)


def local(tiles, tile_counts, doc_order, qkv_weight, out_weight):
    own_tiles = tiles[0, 0]
    return encode_all(tile_counts, doc_order, own_tiles, qkv_weight, out_weight)[None]


def solution(mesh):
    placed = (
        P("dp", "bal", None, "tensor", None),
        P("dp", None),
        P("dp", None),
        P(None, "dp", "tensor"),
        P("dp", "tensor"),
    )
    return jax.shard_map(
        local, mesh=mesh, in_specs=placed, out_specs=P("dp", "bal", "tensor", None), check_vma=False
    )
```

```python
import functools

import jax
import jax.numpy as jnp
from jax import lax
from jax.experimental import pallas as pl
from jax.experimental.pallas import tpu as pltpu
from jax.sharding import PartitionSpec as P

HDIM = 80
CAP = 8
LANES = 128
GROUP = 4
PAIR = 2
EPSILON = 1e-06
LOG2E = 1.4426950408889634
MESH = pl.DeviceIdType.MESH


def flip(index, bit):
    return index + bit - 2 * bit * ((index // bit) % 2)


def bits_of(size):
    bits = []
    while 1 << len(bits) < size:
        bits.append(1 << len(bits))
    return bits


def column_groups(slices):
    width = LANES if slices % LANES == 0 else slices
    return width, slices // width


def pieces_of(slices):
    half = slices // 2
    first = [(0, 0, half), (0, half, half)] if half % 16 == 0 else [(0, 0, slices)]
    return first + [(i, 0, slices) for i in range(1, CAP)]


def remote(src, dst, send, recv, **device):
    return pltpu.make_async_remote_copy(
        src_ref=src, dst_ref=dst, send_sem=send, recv_sem=recv, device_id=device, device_id_type=MESH
    )


def encode_kernel(sizes, *refs):
    nd, nb, nt = sizes
    bits = bits_of(nb)
    ns = len(bits)
    counts, order, tiles_in, wq_in, wo_in, out = refs[:6]
    sends, recvs = refs[6 : 6 + ns], refs[6 + ns : 6 + 2 * ns]
    tiles, gath, wq, wt, wo_own, wo, normed, qkv, ctx, own = refs[6 + 2 * ns : 16 + 2 * ns]
    sems = refs[16 + 2 * ns :]
    t_send, t_recv, y_send, y_recv, c_send, c_recv = sems[:6]
    l_send, l_recv, h_send, h_recv = sems[6:10]
    x_send, x_recv, d_send, d_recv, i_sem = sems[10:]
    z, b, t = lax.axis_index("dp"), lax.axis_index("bal"), lax.axis_index("tensor")
    _, slices, patches = tiles.shape
    width, groups = column_groups(slices)
    pieces = pieces_of(slices)
    per = nd // nt
    features = nt * slices
    kinds = wq.shape[0]
    blocks = CAP // GROUP

    load_tiles = pltpu.make_async_copy(tiles_in, tiles, i_sem.at[0])
    load_q = pltpu.make_async_copy(wq_in, wq.at[:, z], i_sem.at[1])
    load_o = pltpu.make_async_copy(wo_in, wo_own, i_sem.at[2])
    load_tiles.start()
    load_q.start()
    load_o.start()

    barrier = pltpu.get_barrier_semaphore()
    for m in bits:
        pl.semaphore_signal(barrier, inc=1, device_id={"bal": flip(b, m)}, device_id_type=MESH)
    for j in range(1, nt):
        pl.semaphore_signal(barrier, inc=1, device_id={"tensor": (t + j) % nt}, device_id_type=MESH)

    def greet(j, carry):
        pl.semaphore_signal(barrier, inc=1, device_id={"dp": (z + j) % nd}, device_id_type=MESH)
        return carry

    lax.fori_loop(1, nd, greet, 0)

    docs = order.shape[1]
    placed = [order[0, p] for p in range(docs)]
    edges = [jnp.int32(0)]
    for doc in placed:
        edges.append(edges[-1] + counts[0, doc])
    own_start = jnp.int32(0)
    for p in range(docs):
        own_start = own_start + jnp.where(placed[p] == b, edges[p], 0)

    def slot_of(s, r):
        return r >> (s + 1)

    def current(s, r, i, rows):
        block = b
        for m in bits:
            if r & m:
                block = flip(block, m)
        packed = block * CAP + i
        owner = jnp.int32(0)
        for p in range(docs):
            inside = (edges[p] <= packed) & (packed < edges[p + 1])
            owner = owner + jnp.where(inside, placed[p], 0)
        value = tiles[jnp.clip(packed - own_start, 0, tiles.shape[0] - 1), rows]
        for q in range(s):
            apart = (owner // bits[q]) % 2 != (b // bits[q]) % 2
            value = lax.select(apart, recvs[q][slot_of(q, r), i, rows], value)
        return value

    def tile_copy(s, slot, p):
        i, start, count = pieces[p]
        rows = pl.ds(start, count)
        return remote(
            sends[s].at[slot, i, rows],
            recvs[s].at[slot, i, rows],
            t_send.at[s, slot, p],
            t_recv.at[s, slot, p],
            bal=flip(b, bits[s]),
        )

    def wait_for(s, r, p):
        for q in range(s):
            tile_copy(q, slot_of(q, r), p).wait_recv()

    def wanted(s):
        m = bits[s]
        return [r for r in reversed(range(nb)) if r & (m - 1) == 0 and r & m]

    load_tiles.wait()
    for r in wanted(0):
        slot = slot_of(0, r - 1)

        def fill(i, carry, r=r, slot=slot):
            sends[0][slot, i] = current(0, r, i, slice(None))
            return carry

        lax.fori_loop(0, CAP, fill, 0)

    load_o.wait()
    load_q.wait()
    keeper = z // per
    place = z % per

    @pl.when(keeper == t)
    def _():
        wo[t, place, b] = wo_own[b]

    pl.semaphore_wait(barrier, ns + nt - 1 + nd - 1)

    for r in wanted(0):
        for p in range(len(pieces)):
            tile_copy(0, slot_of(0, r - 1), p).start()

    part_count = wq.shape[2]
    part = b % part_count

    def held(src, k):
        src = jnp.clip(src, 0, nd - 1)
        if k == groups:
            return wo.at[:, src % per, b]
        return wq.at[:, src, part, :, pl.ds(k * width, width)]

    def exists(src, k):
        valid = (src >= 0) & (src < nd)
        return valid & (src // per == t) if k == groups else valid

    def line(way, s, k):
        step = 1 - 2 * way
        src = z - step * s
        there = z + step
        at = held(src, k)
        copy = remote(
            at, at, l_send.at[way, s, k], l_recv.at[way, s, k], dp=jnp.clip(there, 0, nd - 1)
        )
        return exists(src, k) & (there >= 0) & (there < nd), copy

    def doubled(q, s, e):
        at = b
        for bit in range(s):
            if (e >> bit) & 1:
                at = flip(at, bits[ns - 1 - bit])
        rows = wo.at[:, q, at]
        index = (1 << s) - 1 + e
        return remote(
            rows, rows, d_send.at[q, index], d_recv.at[q, index], bal=flip(b, bits[ns - 1 - s])
        )

    def arrival(way, s, k):
        step = 1 - 2 * way
        src = z - step * (s + 1)
        at = held(src, k)
        here = remote(
            at, at, l_send.at[way, s, k], l_recv.at[way, s, k], dp=jnp.clip(z + step, 0, nd - 1)
        )
        if k == groups:
            return exists(src, k), here, doubled(jnp.clip(src, 0, nd - 1) % per, 0, 0)
        return (
            exists(src, k),
            here,
            remote(at, at, h_send.at[way, s, k], h_recv.at[way, s, k], bal=flip(b, 1)),
        )

    def begin(ks):
        for k in ks:
            for way in range(2):
                valid, copy = line(way, 0, k)
                pl.when(valid)(copy.start)

    early = min(2, nd - 1)

    def hop(s, k):
        for way in range(2):
            valid, here, half = arrival(way, s, k)
            further, copy = line(way, s + 1, k)

            @pl.when(valid)
            def _(here=here, half=half, further=further, copy=copy):
                here.wait_recv()
                pl.when(further)(copy.start)
                if part_count > 1 or k == groups:
                    half.start()

    def hops(s, ks):
        if s < early:
            for k in ks:
                if k <= groups:
                    hop(s, k)

    def rest(ks):
        for k in ks:
            if k <= groups:

                def one(s, carry, k=k):
                    hop(s, k)
                    return carry

                lax.fori_loop(early, nd - 1, one, 0)

    def halves(s, k):
        for way in range(2):
            valid, _, half = arrival(way, s, k)
            if part_count > 1:
                pl.when(valid)(half.wait_recv)

    first = range(min(3, groups))
    later = range(min(3, groups), groups)
    begin(first)

    def cross(source, target):
        return remote(
            wo_own.at[b], wo.at[source, place, b], x_send.at[0], x_recv.at[source], tensor=target
        )

    @pl.when(keeper != t)
    def _():
        cross(t, keeper).start()

    def spread_out():
        @pl.when(keeper == t)
        def _():
            for j in range(1, nt):
                cross((t + j) % nt, t).wait_recv()
            begin([groups])
            doubled(place, 0, 0).start()

    def finish(s):
        def further(q, carry):
            for e in range(1 << (s - 1)):
                doubled(q, s - 1, e).wait_recv()
            if s < ns:
                for e in range(1 << s):
                    doubled(q, s, e).start()
            return carry

        lax.fori_loop(0, per, further, 0)

    for s in range(1, ns):
        for r in wanted(s):
            slot = slot_of(s, r - bits[s])
            for p, (i, start, count) in enumerate(pieces):
                wait_for(s, r, p)
                rows = pl.ds(start, count)
                sends[s][slot, i, rows] = current(s, r, i, rows)
                tile_copy(s, slot, p).start()

    def y_copy(p, j):
        i, start, count = pieces[p]
        at = gath.at[i, pl.ds(pl.multiple_of(t * slices + start, 16), count), :]
        return remote(at, at, y_send.at[p, j], y_recv.at[p, j], tensor=(t + j) % nt)

    def normalize(i):
        for p, piece in enumerate(pieces):
            if piece[0] == i:
                for j in range(1, nt):
                    y_copy(p, j).wait_recv()
        values = gath[i].astype(jnp.float32)
        center = values - jnp.mean(values, axis=0, keepdims=True)
        spread_of = jnp.mean(center * center, axis=0, keepdims=True)
        normed[:, i * patches : (i + 1) * patches] = (
            center * lax.rsqrt(spread_of + EPSILON)
        ).astype(normed.dtype)

    def ready(k):
        if k >= groups:
            return

        def one(s, carry):
            halves(s, k)
            return carry

        lax.fori_loop(0, nd - 1, one, 0)
        for kind in range(kinds):
            block = wq[kind, :, :, :, k * width : (k + 1) * width].reshape(features, width)
            wt[k, kind * width : (kind + 1) * width, :] = block.T

    def heads_of(k):
        return [h for h in range(slices // HDIM) if k * width < (h + 1) * HDIM <= (k + 1) * width]

    def c_copy(k, n, j):
        first, number = heads_of(k)[0], len(heads_of(k))
        at = ctx.at[
            pl.ds(pl.multiple_of(t * slices + first * HDIM, 16), number * HDIM),
            pl.ds(pl.multiple_of(n * PAIR * patches, patches), PAIR * patches),
        ]
        return remote(at, at, c_send.at[k, n, j], c_recv.at[k, n, j], tensor=(t + j) % nt)

    def columns(i, number):
        return pl.ds(pl.multiple_of(i * patches, patches), number * patches)

    scale = HDIM ** (-0.5) * LOG2E

    def encode(k, g):
        if k >= groups:
            return
        for n in range(0, GROUP, PAIR):
            cols = columns(g * GROUP + n, PAIR)
            result = jnp.dot(wt[k], normed[:, cols], preferred_element_type=jnp.float32)
            for kind in range(kinds):
                qkv[kind, k * width : (k + 1) * width, cols] = result[
                    kind * width : (kind + 1) * width
                ].astype(qkv.dtype)
        for n in range(GROUP):
            cols = columns(g * GROUP + n, 1)
            for h in heads_of(k):
                span = slice(h * HDIM, (h + 1) * HDIM)
                scores = lax.dot_general(
                    qkv[1, span, cols], qkv[0, span, cols], (((0,), (0,)), ((), ())),
                    preferred_element_type=jnp.float32,
                )
                powers = jnp.exp2((scores - jnp.max(scores, axis=0, keepdims=True)) * scale)
                total = jnp.sum(powers, axis=0, keepdims=True)
                value = jnp.dot(
                    qkv[2, span, cols], powers.astype(qkv.dtype), preferred_element_type=jnp.float32
                )
                ctx[pl.ds(pl.multiple_of(t * slices + h * HDIM, 16), HDIM), cols] = (
                    value * (1.0 / total)
                ).astype(ctx.dtype)
        for n in range(GROUP // PAIR):
            for j in range(1, nt):
                c_copy(k, g * (GROUP // PAIR) + n, j).start()

    def both(k):
        if k >= groups:
            return

        def one(g, carry):
            encode(k, g)
            return carry

        lax.fori_loop(0, blocks, one, 0)

    def between(i):
        if i == 0:
            hops(0, [0])
        if i == 1:
            hops(0, first[1:])
        if i == 2:
            hops(1, [0])
        if i == 3:
            hops(1, first[1:2])
        if i == 4:
            hops(1, first[2:])
            begin(later)
        if i == 5:
            rest(first[:2])
        if i == 6:
            hops(0, later)
            spread_out()
            rest(first[2:])
        if i >= 2:
            normalize(i - 2)
        if i == 6:
            ready(0)
            encode(0, 0)
        if i == 7:
            if len(first) > 1:
                ready(1)
                encode(1, 0)

    for p, (i, start, count) in enumerate(pieces):
        wait_for(ns, 0, p)
        rows = pl.ds(start, count)
        gath[i, pl.ds(pl.multiple_of(t * slices + start, 16), count), :] = current(ns, 0, i, rows)
        for j in range(1, nt):
            y_copy(p, j).start()
        if start + count == slices:
            between(i)

    normalize(CAP - 2)
    if len(first) > 2:
        ready(2)
        encode(2, 0)
    hops(1, later)
    normalize(CAP - 1)
    for k in first:
        encode(k, 1)
        if k == 0:
            hops(0, [groups])
    for n, k in enumerate(later):
        rest([k])
        ready(k)
        if n == 1:
            hops(1, [groups])
        both(k)
    if len(later) < 2:
        hops(1, [groups])
    rest([groups])
    for s in range(1, ns + 1):
        finish(s)

    def partial(source, cols):
        weight = wo[source].reshape(slices, slices)
        block = ctx[pl.ds(pl.multiple_of(source * slices, 16), slices), cols]
        return jnp.dot(weight, block, preferred_element_type=jnp.float32).astype(own.dtype)

    for p in range(len(pieces)):
        for j in range(1, nt):
            y_copy(p, j).wait_send()
        for s in range(ns):
            for slot in range(nb >> (s + 1)):
                tile_copy(s, slot, p).wait_send()

    @pl.when(keeper != t)
    def _():
        cross(t, keeper).wait_send()

    def drain_doubled(q, carry):
        for s in range(ns):
            for e in range(1 << s):
                doubled(q, s, e).wait_send()
        return carry

    lax.fori_loop(0, per, drain_doubled, 0)

    def drain_line(s, carry):
        for k in range(groups + 1):
            for way in range(2):
                valid, copy = line(way, s, k)
                pl.when(valid)(copy.wait_send)
                valid, _, half = arrival(way, s, k)
                if part_count > 1 and k < groups:
                    pl.when(valid)(half.wait_send)
        return carry

    lax.fori_loop(0, nd - 1, drain_line, 0)

    def mine(n, carry):
        own[:, columns(PAIR * n, PAIR)] = partial(t, columns(PAIR * n, PAIR))
        return carry

    lax.fori_loop(0, CAP // PAIR, mine, 0)

    def close(n, carry):
        for k in range(groups):
            for j in range(1, nt):
                c_copy(k, n, j).wait_send()
                c_copy(k, n, j).wait_recv()
        i = n * PAIR
        total = own[:, columns(i, PAIR)].astype(jnp.float32)
        for j in range(1, nt):
            total = total + partial((t + j) % nt, columns(i, PAIR)).astype(jnp.float32)
        for e in range(PAIR):
            source = gath[i + e, pl.ds(pl.multiple_of(t * slices, 16), slices), :]
            out[i + e] = (
                source.astype(jnp.float32) + total[:, e * patches : (e + 1) * patches]
            ).astype(out.dtype)
        return carry

    lax.fori_loop(0, CAP // PAIR, close, 0)


def encode_all(counts, ordering, tiles, qkv_weight, out_weight):
    nd, nb, nt = (lax.axis_size(name) for name in ("dp", "bal", "tensor"))
    ns = len(bits_of(nb))
    slots, slices, patches = tiles.shape
    kinds, rows, columns = qkv_weight.shape
    width, groups = column_groups(columns)
    pieces = len(pieces_of(slices))
    per = nd // nt
    wq = qkv_weight.reshape(kinds, min(nb, 2), -1, columns)
    wo = out_weight.reshape(nb, -1, columns)
    dtype = tiles.dtype
    vmem = pl.BlockSpec(memory_space=pltpu.VMEM)
    hbm = pl.BlockSpec(memory_space=pltpu.HBM)
    dma = pltpu.SemaphoreType.DMA

    def space(*shape):
        return pltpu.VMEM(shape, dtype)

    buffers = [space(nb >> (s + 1), CAP, slices, patches) for s in range(ns)]
    return pl.pallas_call(
        functools.partial(encode_kernel, (nd, nb, nt)),
        out_shape=jax.ShapeDtypeStruct((CAP, slices, patches), dtype),
        in_specs=[pl.BlockSpec(memory_space=pltpu.SMEM)] * 2 + [hbm] * 3,
        out_specs=vmem,
        scratch_shapes=buffers
        + buffers
        + [
            space(slots, slices, patches),
            space(CAP, nt * slices, patches),
            space(kinds, nd, *wq.shape[1:]),
            space(groups, kinds * width, nt * slices),
            space(*wo.shape),
            space(nt, per, *wo.shape),
            space(nt * slices, CAP * patches),
            space(kinds, columns, CAP * patches),
            space(nt * slices, CAP * patches),
            space(slices, CAP * patches),
        ]
        + [dma((ns, max(nb // 2, 1), pieces))] * 2
        + [dma((pieces, nt))] * 2
        + [dma((groups, CAP // PAIR, nt))] * 2
        + [dma((2, nd, groups + 1))] * 4
        + [dma((1,)), dma((nt,))]
        + [dma((per, nb))] * 2
        + [dma((3,))],
        compiler_params=pltpu.CompilerParams(
            collective_id=0, has_side_effects=True, vmem_limit_bytes=44 * 1024 * 1024
        ),
        name="encode_all",
    )(*(pltpu.with_memory_space_constraint(a, pltpu.HBM) for a in (counts, ordering, tiles, wq, wo)))


def local(tiles, tile_counts, doc_order, qkv_weight, out_weight):
    own_tiles = tiles[0, 0]
    return encode_all(tile_counts, doc_order, own_tiles, qkv_weight, out_weight)[None]


def solution(mesh):
    placed = (
        P("dp", "bal", None, "tensor", None),
        P("dp", None),
        P("dp", None),
        P(None, "dp", "tensor"),
        P("dp", "tensor"),
    )
    return jax.shard_map(
        local, mesh=mesh, in_specs=placed, out_specs=P("dp", "bal", "tensor", None), check_vma=False
    )
```

```python
import functools

import jax
import jax.numpy as jnp
from jax import lax
from jax.experimental import pallas as pl
from jax.experimental.pallas import tpu as pltpu
from jax.sharding import PartitionSpec as P

HDIM = 80
CAP = 8
LANES = 128
GROUP = 4
PAIR = 2
HALVES = 2
EPSILON = 1e-06
LOG2E = 1.4426950408889634
MESH = pl.DeviceIdType.MESH


def flip(index, bit):
    return index + bit - 2 * bit * ((index // bit) % 2)


def bits_of(size):
    bits = []
    while 1 << len(bits) < size:
        bits.append(1 << len(bits))
    return bits


def column_groups(slices):
    width = LANES if slices % LANES == 0 else slices
    return width, slices // width


def pieces_of(slices, parts):
    part = slices // parts if slices % (16 * parts) == 0 else slices
    return [(i, start, part) for i in range(CAP) for start in range(0, slices, part)]


def remote(src, dst, send, recv, **device):
    return pltpu.make_async_remote_copy(
        src_ref=src, dst_ref=dst, send_sem=send, recv_sem=recv, device_id=device, device_id_type=MESH
    )


def encode_kernel(sizes, *refs):
    nd, nb, nt = sizes
    bits = bits_of(nb)
    ns = len(bits)
    counts_in, order_in, tiles_in, wq_in, wo_in, out = refs[:6]
    sends, recvs = refs[6 : 6 + ns], refs[6 + ns : 6 + 2 * ns]
    tiles, gath, wq, wt, wo_own, wo, normed, qkv, ctx, own, counts, order = refs[
        6 + 2 * ns : 18 + 2 * ns
    ]
    t_recv = refs[18 + 2 * ns : 18 + 3 * ns]
    t_send, y_send, y_recv, c_send, c_recv, l_send, l_recv, h_send, h_recv = refs[
        18 + 3 * ns : 27 + 3 * ns
    ]
    x_send, x_recv, d_send, d_recv, e_recv, i_sem = refs[27 + 3 * ns :]
    z, b, t = lax.axis_index("dp"), lax.axis_index("bal"), lax.axis_index("tensor")
    _, slices, patches = tiles.shape
    width, groups = column_groups(slices)
    pieces = [pieces_of(slices, HALVES if s == ns - 1 else 1) for s in range(ns)]
    per = nd // nt
    features = nt * slices
    kinds = wq.shape[0]
    blocks = CAP // GROUP

    barrier = pltpu.get_barrier_semaphore()
    for m in bits:
        pl.semaphore_signal(barrier, inc=1, device_id={"bal": flip(b, m)}, device_id_type=MESH)
    for j in range(1, nt):
        pl.semaphore_signal(barrier, inc=1, device_id={"tensor": (t + j) % nt}, device_id_type=MESH)

    def greet(j, carry):
        pl.semaphore_signal(barrier, inc=1, device_id={"dp": (z + j) % nd}, device_id_type=MESH)
        return carry

    lax.fori_loop(1, nd, greet, 0)

    load_counts = pltpu.make_async_copy(counts_in, counts, i_sem.at[3])
    load_order = pltpu.make_async_copy(order_in, order, i_sem.at[4])
    load_tiles = pltpu.make_async_copy(tiles_in, tiles, i_sem.at[0])
    load_q = pltpu.make_async_copy(wq_in, wq.at[:, z], i_sem.at[1])
    load_o = pltpu.make_async_copy(wo_in, wo_own, i_sem.at[2])
    load_counts.start()
    load_order.start()
    load_tiles.start()
    load_o.start()
    load_q.start()
    load_counts.wait()
    load_order.wait()

    docs = order.shape[1]
    placed = [order[0, p] for p in range(docs)]
    edges = [jnp.int32(0)]
    for doc in placed:
        edges.append(edges[-1] + counts[0, doc])
    own_start = jnp.int32(0)
    for p in range(docs):
        own_start = own_start + jnp.where(placed[p] == b, edges[p], 0)

    def slot_of(s, r):
        return r >> (s + 1)

    def current(s, r, i, rows):
        block = b
        for m in bits:
            if r & m:
                block = flip(block, m)
        packed = block * CAP + i
        owner = jnp.int32(0)
        for p in range(docs):
            inside = (edges[p] <= packed) & (packed < edges[p + 1])
            owner = owner + jnp.where(inside, placed[p], 0)
        value = tiles[jnp.clip(packed - own_start, 0, tiles.shape[0] - 1), rows]
        for q in range(s):
            apart = (owner // bits[q]) % 2 != (b // bits[q]) % 2
            value = lax.select(apart, recvs[q][slot_of(q, r), i, rows], value)
        return value

    def tile_copy(s, slot, p):
        i, start, count = pieces[s][p]
        rows = pl.ds(start, count)
        return remote(
            sends[s].at[slot, i, rows],
            recvs[s].at[slot, i, rows],
            t_send.at[s, slot],
            t_recv[s].at[slot, p],
            bal=flip(b, bits[s]),
        )

    def wait_for(s, r, piece):
        i, start, count = piece
        for q in range(s):
            for p, (tile, first, number) in enumerate(pieces[q]):
                if tile == i and start <= first < start + count:
                    tile_copy(q, slot_of(q, r), p).wait_recv()

    def wanted(s):
        m = bits[s]
        return [r for r in reversed(range(nb)) if r & (m - 1) == 0 and r & m]

    load_tiles.wait()
    for r in wanted(0):
        slot = slot_of(0, r - 1)

        def fill(i, carry, r=r, slot=slot):
            sends[0][slot, i] = current(0, r, i, slice(None))
            return carry

        lax.fori_loop(0, CAP, fill, 0)

    load_o.wait()
    load_q.wait()
    keeper = z // per
    place = z % per

    @pl.when(keeper == t)
    def _():
        wo[t, place, b] = wo_own[b]

    pl.semaphore_wait(barrier, ns + nt - 1 + nd - 1)

    for r in wanted(0):
        for p in range(len(pieces[0])):
            tile_copy(0, slot_of(0, r - 1), p).start()

    part_count = wq.shape[2]
    part = b % part_count

    def held(src, k):
        src = jnp.clip(src, 0, nd - 1)
        if k == groups:
            return wo.at[:, src % per, b]
        return wq.at[:, src, part, :, pl.ds(k * width, width)]

    def exists(src, k):
        valid = (src >= 0) & (src < nd)
        return valid & (src // per == t) if k == groups else valid

    def line(way, s, k):
        step = 1 - 2 * way
        src = z - step * s
        there = z + step
        at = held(src, k)
        at_step = min(s, nd - 2) if isinstance(s, int) else jnp.minimum(s, nd - 2)
        copy = remote(
            at, at, l_send.at[way, at_step, int(k == groups)], l_recv.at[way, at_step, k],
            dp=jnp.clip(there, 0, nd - 1),
        )
        return exists(src, k) & (there >= 0) & (there < nd), copy

    def doubled(q, s, e):
        at = b
        for bit in range(s):
            if (e >> bit) & 1:
                at = flip(at, bits[ns - 1 - bit])
        rows = wo.at[:, q, at]
        landed = e_recv.at[s] if s else d_recv.at[q]
        return remote(rows, rows, d_send.at[0], landed, bal=flip(b, bits[ns - 1 - s]))

    def arrival(way, s, k):
        step = 1 - 2 * way
        src = z - step * (s + 1)
        at = held(src, k)
        here = remote(
            at, at, l_send.at[way, s, 0], l_recv.at[way, s, k], dp=jnp.clip(z + step, 0, nd - 1)
        )
        if k == groups:
            return exists(src, k), here, doubled(jnp.clip(src, 0, nd - 1) % per, 0, 0)
        return (
            exists(src, k),
            here,
            remote(at, at, h_send.at[0], h_recv.at[k], bal=flip(b, 1)),
        )

    def begin(ks):
        for k in ks:
            for way in range(2):
                valid, copy = line(way, 0, k)
                pl.when(valid)(copy.start)

    early = min(2, nd - 1)

    def hop(s, k, onward):
        for way in range(2):
            valid, here, half = arrival(way, s, k)
            further, copy = line(way, s + 1, k)

            @pl.when(valid & (further if onward else jnp.logical_not(further)))
            def _(here=here, half=half, copy=copy):
                here.wait_recv()
                if onward:
                    copy.start()
                if part_count > 1 or k == groups:
                    half.start()

    def forward(s, ks):
        if s < early:
            for k in ks:
                if k <= groups:
                    hop(s, k, True)

    def accept(s, ks):
        if s < early:
            for k in ks:
                if k <= groups:
                    hop(s, k, False)

    def rest(ks):
        for k in ks:
            if k <= groups:

                def one(s, carry, k=k):
                    hop(s, k, True)
                    hop(s, k, False)
                    return carry

                lax.fori_loop(early, nd - 1, one, 0)

    first = range(min(3, groups))
    later = range(min(3, groups), groups)
    begin(first)

    def cross(source, target):
        return remote(
            wo_own.at[b], wo.at[source, place, b], x_send.at[0], x_recv.at[source], tensor=target
        )

    @pl.when(keeper != t)
    def _():
        cross(t, keeper).start()

    def spread_out():
        @pl.when(keeper == t)
        def _():
            for j in range(1, nt):
                cross((t + j) % nt, t).wait_recv()
            begin([groups])
            doubled(place, 0, 0).start()

    def finish(s):
        def further(q, carry):
            if s == 1:
                doubled(q, 0, 0).wait_recv()
            if s < ns:
                for e in range(1 << s):
                    doubled(q, s, e).start()
            return carry

        if s > 1:
            at = wo.at[:, :, pl.ds(0, 1 << (s - 1))]
            remote(at, at, d_send.at[0], e_recv.at[s - 1], bal=flip(b, bits[ns - s])).wait_recv()
        if s < ns or s == 1:
            lax.fori_loop(0, per, further, 0)

    for s in range(1, ns):
        for r in wanted(s):
            slot = slot_of(s, r - bits[s])
            for p, (i, start, count) in enumerate(pieces[s]):
                wait_for(s, r, pieces[s][p])
                rows = pl.ds(start, count)
                sends[s][slot, i, rows] = current(s, r, i, rows)
                tile_copy(s, slot, p).start()

    fine = pieces[ns - 1]

    def y_copy(i, start, count, j):
        at = gath.at[i, pl.ds(pl.multiple_of(t * slices + start, 16), count), :]
        return remote(at, at, y_send.at[j - 1], y_recv.at[i, j - 1], tensor=(t + j) % nt)

    def normalize(i):
        for j in range(1, nt):
            y_copy(i, 0, slices, j).wait_recv()
        values = gath[i].astype(jnp.float32)
        center = values - jnp.mean(values, axis=0, keepdims=True)
        spread_of = jnp.mean(center * center, axis=0, keepdims=True)
        normed[:, i * patches : (i + 1) * patches] = (
            center * lax.rsqrt(spread_of + EPSILON)
        ).astype(normed.dtype)

    def ready(k):
        if k >= groups:
            return

        if part_count > 1:
            at = wq.at[:, pl.ds(0, nd - 1), part, :, pl.ds(k * width, width)]
            remote(at, at, h_send.at[0], h_recv.at[k], bal=flip(b, 1)).wait_recv()
        for kind in range(kinds):
            block = wq[kind, :, :, :, k * width : (k + 1) * width].reshape(features, width)
            wt[k, kind * width : (kind + 1) * width, :] = block.T

    def heads_of(k):
        return [h for h in range(slices // HDIM) if k * width < (h + 1) * HDIM <= (k + 1) * width]

    def c_copy(k, n, j):
        first, number = heads_of(k)[0], len(heads_of(k))
        at = ctx.at[
            pl.ds(pl.multiple_of(t * slices + first * HDIM, 16), number * HDIM),
            pl.ds(pl.multiple_of(n * PAIR * patches, patches), PAIR * patches),
        ]
        return remote(at, at, c_send.at[j - 1], c_recv.at[n, j - 1], tensor=(t + j) % nt)

    def columns(i, number):
        return pl.ds(pl.multiple_of(i * patches, patches), number * patches)

    scale = HDIM ** (-0.5) * LOG2E

    def encode(k, g):
        if k >= groups:
            return
        for n in range(0, GROUP, PAIR):
            cols = columns(g * GROUP + n, PAIR)
            result = jnp.dot(wt[k], normed[:, cols], preferred_element_type=jnp.float32)
            for kind in range(kinds):
                qkv[kind, k * width : (k + 1) * width, cols] = result[
                    kind * width : (kind + 1) * width
                ].astype(qkv.dtype)
        for n in range(GROUP):
            cols = columns(g * GROUP + n, 1)
            for h in heads_of(k):
                span = slice(h * HDIM, (h + 1) * HDIM)
                scores = lax.dot_general(
                    qkv[1, span, cols], qkv[0, span, cols], (((0,), (0,)), ((), ())),
                    preferred_element_type=jnp.float32,
                )
                powers = jnp.exp2((scores - jnp.max(scores, axis=0, keepdims=True)) * scale)
                total = jnp.sum(powers, axis=0, keepdims=True)
                value = jnp.dot(
                    qkv[2, span, cols], powers.astype(qkv.dtype), preferred_element_type=jnp.float32
                )
                ctx[pl.ds(pl.multiple_of(t * slices + h * HDIM, 16), HDIM), cols] = (
                    value * (1.0 / total)
                ).astype(ctx.dtype)
        for n in range(GROUP // PAIR):
            for j in range(1, nt):
                c_copy(k, g * (GROUP // PAIR) + n, j).start()

    def both(k):
        if k >= groups:
            return

        def one(g, carry):
            encode(k, g)
            return carry

        lax.fori_loop(0, blocks, one, 0)

    last = [groups]
    steps = {
        0: lambda: forward(0, [0]),
        2: lambda: forward(0, first[1:2]),
        3: lambda: forward(0, first[2:]),
        5: lambda: forward(1, [0]),
        6: lambda: forward(1, first[1:2]),
        8: lambda: (forward(1, first[2:]), begin(later)),
        9: lambda: (accept(0, first), accept(1, first)),
        11: lambda: forward(0, later[:1]),
        12: lambda: (forward(0, later[1:]), rest(first)),
        13: spread_out,
        14: lambda: (forward(1, later[:1]), ready(0), encode(0, 0)),
        15: lambda: forward(1, later[1:]),
    }
    count_of = len(fine)
    for p, (i, start, count) in enumerate(fine):
        wait_for(ns, 0, (i, start, count))
        rows = pl.ds(start, count)
        gath[i, pl.ds(pl.multiple_of(t * slices + start, 16), count), :] = current(ns, 0, i, rows)
        for j in range(1, nt):
            y_copy(i, start, count, j).start()
        for at in range(2 * CAP):
            if at * count_of // (2 * CAP) == p and at in steps:
                steps[at]()
        if start + count == slices and i >= 2:
            normalize(i - 2)

    ready(1)
    encode(1, 0)
    normalize(CAP - 2)
    accept(0, later)
    ready(2)
    encode(2, 0)
    forward(0, last)
    normalize(CAP - 1)
    encode(0, 1)
    accept(1, later)
    encode(1, 1)
    forward(1, last)
    rest(later)
    encode(2, 1)
    for k in later:
        ready(k)
        if k < groups - 1:
            both(k)
    if later:
        encode(later[-1], 0)
    accept(0, last)
    accept(1, last)
    rest(last)
    if later:
        encode(later[-1], 1)

    def partial(source, cols):
        weight = wo[source].reshape(slices, slices)
        block = ctx[pl.ds(pl.multiple_of(source * slices, 16), slices), cols]
        return jnp.dot(weight, block, preferred_element_type=jnp.float32).astype(own.dtype)

    for j in range(1, nt):
        at = gath.at[:, pl.ds(0, slices), :]
        remote(at, at, y_send.at[j - 1], y_recv.at[0, j - 1], tensor=(t + j) % nt).wait_send()
    for s in range(ns):
        for slot in range(nb >> (s + 1)):
            remote(
                sends[s].at[slot], recvs[s].at[slot], t_send.at[s, slot], t_recv[s].at[slot, 0],
                bal=flip(b, bits[s]),
            ).wait_send()

    @pl.when(keeper != t)
    def _():
        cross(t, keeper).wait_send()

    def drain_line(s, carry):
        for way in range(2):
            step = 1 - 2 * way
            src = z - step * s
            there = z + step
            goes = (there >= 0) & (there < nd)
            at = wq.at[:, jnp.clip(src, 0, nd - 1), part]
            copy = remote(
                at, at, l_send.at[way, s, 0], l_recv.at[way, s, 0], dp=jnp.clip(there, 0, nd - 1)
            )
            pl.when(exists(src, 0) & goes)(copy.wait_send)
            valid, copy = line(way, s, groups)
            pl.when(valid)(copy.wait_send)
        return carry

    lax.fori_loop(0, nd - 1, drain_line, 0)
    if part_count > 1:
        at = wq.at[:, pl.ds(0, nd - 1), part]
        remote(at, at, h_send.at[0], h_recv.at[0], bal=flip(b, 1)).wait_send()

    for s in range(1, ns + 1):
        finish(s)

    at = wo.at[:, :, pl.ds(0, nb - 1)]
    remote(at, at, d_send.at[0], d_recv.at[0], bal=flip(b, 1)).wait_send()

    def mine(n, carry):
        own[:, columns(PAIR * n, PAIR)] = partial(t, columns(PAIR * n, PAIR))
        return carry

    lax.fori_loop(0, CAP // PAIR, mine, 0)

    def close(n, carry):
        i = n * PAIR
        for j in range(1, nt):
            at = ctx.at[pl.ds(0, slices), columns(i, PAIR)]
            arrived = remote(at, at, c_send.at[j - 1], c_recv.at[n, j - 1], tensor=(t + j) % nt)
            arrived.wait_recv()
        total = own[:, columns(i, PAIR)].astype(jnp.float32)
        for j in range(1, nt):
            total = total + partial((t + j) % nt, columns(i, PAIR)).astype(jnp.float32)
        for e in range(PAIR):
            source = gath[i + e, pl.ds(pl.multiple_of(t * slices, 16), slices), :]
            out[i + e] = (
                source.astype(jnp.float32) + total[:, e * patches : (e + 1) * patches]
            ).astype(out.dtype)
        return carry

    lax.fori_loop(0, CAP // PAIR, close, 0)
    for j in range(1, nt):
        at = ctx.at[pl.ds(0, slices), :]
        remote(at, at, c_send.at[j - 1], c_recv.at[0, j - 1], tensor=(t + j) % nt).wait_send()


def encode_all(counts, ordering, tiles, qkv_weight, out_weight):
    nd, nb, nt = (lax.axis_size(name) for name in ("dp", "bal", "tensor"))
    ns = len(bits_of(nb))
    slots, slices, patches = tiles.shape
    kinds, rows, columns = qkv_weight.shape
    width, groups = column_groups(columns)
    per = nd // nt
    wq = qkv_weight.reshape(kinds, min(nb, 2), -1, columns)
    wo = out_weight.reshape(nb, -1, columns)
    dtype = tiles.dtype
    vmem = pl.BlockSpec(memory_space=pltpu.VMEM)
    hbm = pl.BlockSpec(memory_space=pltpu.HBM)
    dma = pltpu.SemaphoreType.DMA

    def space(*shape):
        return pltpu.VMEM(shape, dtype)

    buffers = [space(nb >> (s + 1), CAP, slices, patches) for s in range(ns)]
    return pl.pallas_call(
        functools.partial(encode_kernel, (nd, nb, nt)),
        out_shape=jax.ShapeDtypeStruct((CAP, slices, patches), dtype),
        in_specs=[hbm] * 5,
        out_specs=vmem,
        scratch_shapes=buffers
        + buffers
        + [
            space(slots, slices, patches),
            space(CAP, nt * slices, patches),
            space(kinds, nd, *wq.shape[1:]),
            space(groups, kinds * width, nt * slices),
            space(*wo.shape),
            space(nt, per, *wo.shape),
            space(nt * slices, CAP * patches),
            space(kinds, columns, CAP * patches),
            space(nt * slices, CAP * patches),
            space(slices, CAP * patches),
        ]
        + [pltpu.SMEM(counts.shape, counts.dtype), pltpu.SMEM(ordering.shape, ordering.dtype)]
        + [
            dma((nb >> (s + 1), len(pieces_of(slices, HALVES if s == ns - 1 else 1))))
            for s in range(ns)
        ]
        + [dma((ns, max(nb // 2, 1))), dma((nt - 1,)), dma((CAP, nt - 1))]
        + [dma((nt - 1,)), dma((CAP // PAIR, nt - 1))]
        + [dma((2, nd - 1, 2)), dma((2, nd - 1, groups + 1)), dma((1,)), dma((groups,))]
        + [dma((1,)), dma((nt,)), dma((1,)), dma((per,)), dma((ns,)), dma((5,))],
        compiler_params=pltpu.CompilerParams(
            collective_id=0, has_side_effects=True, vmem_limit_bytes=44 * 1024 * 1024
        ),
        name="encode_all",
    )(*(pltpu.with_memory_space_constraint(a, pltpu.HBM) for a in (counts, ordering, tiles, wq, wo)))


def local(tiles, tile_counts, doc_order, qkv_weight, out_weight):
    own_tiles = tiles[0, 0]
    return encode_all(tile_counts, doc_order, own_tiles, qkv_weight, out_weight)[None]


def solution(mesh):
    placed = (
        P("dp", "bal", None, "tensor", None),
        P("dp", None),
        P("dp", None),
        P(None, "dp", "tensor"),
        P("dp", "tensor"),
    )
    return jax.shard_map(
        local, mesh=mesh, in_specs=placed, out_specs=P("dp", "bal", "tensor", None), check_vma=False
    )
```

```python
import functools

import jax
import jax.numpy as jnp
from jax import lax
from jax.experimental import pallas as pl
from jax.experimental.pallas import tpu as pltpu
from jax.sharding import PartitionSpec as P

HDIM = 80
CAP = 8
LANES = 128
GROUP = 4
PAIR = 2
QUARTERS = 4
EPSILON = 1e-06
LOG2E = 1.4426950408889634
MESH = pl.DeviceIdType.MESH


def flip(index, bit):
    return index + bit - 2 * bit * ((index // bit) % 2)


def bits_of(size):
    bits = []
    while 1 << len(bits) < size:
        bits.append(1 << len(bits))
    return bits


def column_groups(slices):
    width = LANES if slices % LANES == 0 else slices
    return width, slices // width


def pieces_of(slices, parts):
    part = slices // parts if slices % (16 * parts) == 0 else slices
    return [(i, start, part) for i in range(CAP) for start in range(0, slices, part)]


def waves_of(groups):
    waves, start = [], 0
    for count in (1, 2):
        if start + count < groups:
            waves.append((start, count))
            start += count
    return waves + [(start, groups - start)]


def remote(src, dst, send, recv, **device):
    return pltpu.make_async_remote_copy(
        src_ref=src, dst_ref=dst, send_sem=send, recv_sem=recv, device_id=device, device_id_type=MESH
    )


def encode_kernel(sizes, *refs):
    nd, nb, nt = sizes
    bits = bits_of(nb)
    ns = len(bits)
    counts_in, order_in, tiles_in, wq_in, wo_in, out = refs[:6]
    sends, recvs = refs[6 : 6 + ns], refs[6 + ns : 6 + 2 * ns]
    tiles, gath, wq, wt, wo_own, wo, normed, qkv, ctx, own, counts, order = refs[
        6 + 2 * ns : 18 + 2 * ns
    ]
    t_recv = refs[18 + 2 * ns : 18 + 3 * ns]
    t_send, y_send, y_recv, c_send, c_recv, l_send, l_recv, h_send, h_recv = refs[
        18 + 3 * ns : 27 + 3 * ns
    ]
    x_send, x_recv, d_send, d_recv, e_recv, i_sem = refs[27 + 3 * ns :]
    z, b, t = lax.axis_index("dp"), lax.axis_index("bal"), lax.axis_index("tensor")
    _, slices, patches = tiles.shape
    width, groups = column_groups(slices)
    waves = waves_of(groups)
    final = len(waves)
    pieces = [pieces_of(slices, QUARTERS if s == ns - 1 else 1) for s in range(ns)]
    per = nd // nt
    features = nt * slices
    kinds = wq.shape[0]
    blocks = CAP // GROUP

    barrier = pltpu.get_barrier_semaphore()
    for m in bits:
        pl.semaphore_signal(barrier, inc=1, device_id={"bal": flip(b, m)}, device_id_type=MESH)
    for j in range(1, nt):
        pl.semaphore_signal(barrier, inc=1, device_id={"tensor": (t + j) % nt}, device_id_type=MESH)

    for step in (-1, 1):

        @pl.when((z + step >= 0) & (z + step < nd))
        def _(step=step):
            there = jnp.clip(z + step, 0, nd - 1)
            pl.semaphore_signal(barrier, inc=1, device_id={"dp": there}, device_id_type=MESH)

    greeted = jnp.int32(z > 0) + jnp.int32(z < nd - 1)

    load_counts = pltpu.make_async_copy(counts_in, counts, i_sem.at[3])
    load_order = pltpu.make_async_copy(order_in, order, i_sem.at[4])
    load_tiles = pltpu.make_async_copy(tiles_in, tiles, i_sem.at[0])
    load_q = pltpu.make_async_copy(wq_in, wq.at[:, z], i_sem.at[1])
    load_o = pltpu.make_async_copy(wo_in, wo_own, i_sem.at[2])
    load_counts.start()
    load_order.start()
    load_tiles.start()
    load_counts.wait()
    load_order.wait()

    docs = order.shape[1]
    placed = [order[0, p] for p in range(docs)]
    edges = [jnp.int32(0)]
    for doc in placed:
        edges.append(edges[-1] + counts[0, doc])
    own_start = jnp.int32(0)
    for p in range(docs):
        own_start = own_start + jnp.where(placed[p] == b, edges[p], 0)

    def slot_of(s, r):
        return r >> (s + 1)

    def current(s, r, i, rows):
        block = b
        for m in bits:
            if r & m:
                block = flip(block, m)
        packed = block * CAP + i
        owner = jnp.int32(0)
        for p in range(docs):
            inside = (edges[p] <= packed) & (packed < edges[p + 1])
            owner = owner + jnp.where(inside, placed[p], 0)
        value = tiles[jnp.clip(packed - own_start, 0, tiles.shape[0] - 1), rows]
        for q in range(s):
            apart = (owner // bits[q]) % 2 != (b // bits[q]) % 2
            value = lax.select(apart, recvs[q][slot_of(q, r), i, rows], value)
        return value

    def tile_copy(s, slot, p):
        i, start, count = pieces[s][p]
        rows = pl.ds(start, count)
        return remote(
            sends[s].at[slot, i, rows],
            recvs[s].at[slot, i, rows],
            t_send.at[s, slot],
            t_recv[s].at[slot, p],
            bal=flip(b, bits[s]),
        )

    def wait_for(s, r, piece):
        i, start, count = piece
        for q in range(s):
            for p, (tile, first, number) in enumerate(pieces[q]):
                if tile == i and start <= first < start + count:
                    tile_copy(q, slot_of(q, r), p).wait_recv()

    def wanted(s):
        m = bits[s]
        return [r for r in reversed(range(nb)) if r & (m - 1) == 0 and r & m]

    load_tiles.wait()
    load_q.start()
    load_o.start()
    for r in wanted(0):
        slot = slot_of(0, r - 1)

        def fill(i, carry, r=r, slot=slot):
            sends[0][slot, i] = current(0, r, i, slice(None))
            return carry

        lax.fori_loop(0, CAP, fill, 0)

    pl.semaphore_wait(barrier, ns + nt - 1 + greeted)

    for r in wanted(0):
        for p in range(len(pieces[0])):
            tile_copy(0, slot_of(0, r - 1), p).start()

    load_o.wait()
    load_q.wait()
    keeper = z // per
    place = z % per

    @pl.when(keeper == t)
    def _():
        wo[t, place, b] = wo_own[b]

    part_count = wq.shape[2]
    part = b % part_count

    def held(src, w):
        src = jnp.clip(src, 0, nd - 1)
        if w == final:
            return wo.at[:, src % per, b]
        start, count = waves[w]
        return wq.at[:, src, part, :, pl.ds(start * width, count * width)]

    def exists(src, w):
        valid = (src >= 0) & (src < nd)
        return valid & (src // per == t) if w == final else valid

    def line(way, s, w):
        step = 1 - 2 * way
        src = z - step * s
        there = z + step
        at = held(src, w)
        at_step = min(s, nd - 2) if isinstance(s, int) else jnp.minimum(s, nd - 2)
        copy = remote(
            at, at, l_send.at[way, at_step, int(w == final)], l_recv.at[way, at_step, w],
            dp=jnp.clip(there, 0, nd - 1),
        )
        return exists(src, w) & (there >= 0) & (there < nd), copy

    def doubled(q, s, e):
        at = b
        for bit in range(s):
            if (e >> bit) & 1:
                at = flip(at, bits[ns - 1 - bit])
        rows = wo.at[:, q, at]
        landed = e_recv.at[s] if s else d_recv.at[q]
        return remote(rows, rows, d_send.at[0], landed, bal=flip(b, bits[ns - 1 - s]))

    def arrival(way, s, w):
        step = 1 - 2 * way
        src = z - step * (s + 1)
        at = held(src, w)
        here = remote(
            at, at, l_send.at[way, s, 0], l_recv.at[way, s, w], dp=jnp.clip(z + step, 0, nd - 1)
        )
        if w == final:
            return exists(src, w), here, doubled(jnp.clip(src, 0, nd - 1) % per, 0, 0)
        return exists(src, w), here, remote(at, at, h_send.at[0], h_recv.at[w], bal=flip(b, 1))

    def begin(w):
        for way in range(2):
            valid, copy = line(way, 0, w)
            pl.when(valid)(copy.start)

    early = min(2, nd - 1)

    def hop(s, w, onward):
        for way in range(2):
            valid, here, half = arrival(way, s, w)
            further, copy = line(way, s + 1, w)

            @pl.when(valid & (further if onward else jnp.logical_not(further)))
            def _(here=here, half=half, copy=copy):
                here.wait_recv()
                if onward:
                    copy.start()
                if part_count > 1 or w == final:
                    half.start()

    def forward(s, w):
        if s < early and w <= final:
            hop(s, w, True)

    def accept(s, w):
        if s < early and w <= final:
            hop(s, w, False)

    def rest(w):
        def one(s, carry):
            hop(s, w, True)
            hop(s, w, False)
            return carry

        if w <= final:
            lax.fori_loop(early, nd - 1, one, 0)

    for w in range(min(2, final)):
        begin(w)

    def cross(source, target):
        return remote(
            wo_own.at[b], wo.at[source, place, b], x_send.at[0], x_recv.at[source], tensor=target
        )

    @pl.when(keeper != t)
    def _():
        cross(t, keeper).start()

    def spread_out():
        @pl.when(keeper == t)
        def _():
            for j in range(1, nt):
                cross((t + j) % nt, t).wait_recv()
            begin(final)
            doubled(place, 0, 0).start()

    def finish(s):
        def further(q, carry):
            if s == 1:
                doubled(q, 0, 0).wait_recv()
            if s < ns:
                for e in range(1 << s):
                    doubled(q, s, e).start()
            return carry

        if s > 1:
            at = wo.at[:, :, pl.ds(0, 1 << (s - 1))]
            remote(at, at, d_send.at[0], e_recv.at[s - 1], bal=flip(b, bits[ns - s])).wait_recv()
        if s < ns or s == 1:
            lax.fori_loop(0, per, further, 0)

    for s in range(1, ns):
        for r in wanted(s):
            slot = slot_of(s, r - bits[s])
            for p, (i, start, count) in enumerate(pieces[s]):
                wait_for(s, r, pieces[s][p])
                rows = pl.ds(start, count)
                sends[s][slot, i, rows] = current(s, r, i, rows)
                tile_copy(s, slot, p).start()

    fine = pieces[ns - 1]

    def y_copy(i, start, count, j):
        at = gath.at[i, pl.ds(pl.multiple_of(t * slices + start, 16), count), :]
        return remote(at, at, y_send.at[j - 1], y_recv.at[i, j - 1], tensor=(t + j) % nt)

    def normalize(i):
        for j in range(1, nt):
            y_copy(i, 0, slices, j).wait_recv()
        values = gath[i].astype(jnp.float32)
        center = values - jnp.mean(values, axis=0, keepdims=True)
        spread_of = jnp.mean(center * center, axis=0, keepdims=True)
        normed[:, i * patches : (i + 1) * patches] = (
            center * lax.rsqrt(spread_of + EPSILON)
        ).astype(normed.dtype)

    def ready(k):
        if k >= groups:
            return

        for w, (start, count) in enumerate(waves):
            if part_count > 1 and start == k:
                at = wq.at[:, pl.ds(0, nd - 1), part, :, pl.ds(start * width, count * width)]
                remote(at, at, h_send.at[0], h_recv.at[w], bal=flip(b, 1)).wait_recv()
        for kind in range(kinds):
            block = wq[kind, :, :, :, k * width : (k + 1) * width].reshape(features, width)
            wt[k, kind * width : (kind + 1) * width, :] = block.T

    def heads_of(k):
        return [h for h in range(slices // HDIM) if k * width < (h + 1) * HDIM <= (k + 1) * width]

    def c_copy(k, n, j):
        first, number = heads_of(k)[0], len(heads_of(k))
        at = ctx.at[
            pl.ds(pl.multiple_of(t * slices + first * HDIM, 16), number * HDIM),
            pl.ds(pl.multiple_of(n * PAIR * patches, patches), PAIR * patches),
        ]
        return remote(at, at, c_send.at[j - 1], c_recv.at[n, j - 1], tensor=(t + j) % nt)

    def columns(i, number):
        return pl.ds(pl.multiple_of(i * patches, patches), number * patches)

    scale = HDIM ** (-0.5) * LOG2E

    def encode(k, g):
        if k >= groups:
            return
        for n in range(0, GROUP, PAIR):
            cols = columns(g * GROUP + n, PAIR)
            result = jnp.dot(wt[k], normed[:, cols], preferred_element_type=jnp.float32)
            for kind in range(kinds):
                qkv[kind, k * width : (k + 1) * width, cols] = result[
                    kind * width : (kind + 1) * width
                ].astype(qkv.dtype)
        for n in range(GROUP):
            cols = columns(g * GROUP + n, 1)
            for h in heads_of(k):
                span = slice(h * HDIM, (h + 1) * HDIM)
                scores = lax.dot_general(
                    qkv[1, span, cols], qkv[0, span, cols], (((0,), (0,)), ((), ())),
                    preferred_element_type=jnp.float32,
                )
                powers = jnp.exp2((scores - jnp.max(scores, axis=0, keepdims=True)) * scale)
                total = jnp.sum(powers, axis=0, keepdims=True)
                value = jnp.dot(
                    qkv[2, span, cols], powers.astype(qkv.dtype), preferred_element_type=jnp.float32
                )
                ctx[pl.ds(pl.multiple_of(t * slices + h * HDIM, 16), HDIM), cols] = (
                    value * (1.0 / total)
                ).astype(ctx.dtype)
        for n in range(GROUP // PAIR):
            for j in range(1, nt):
                c_copy(k, g * (GROUP // PAIR) + n, j).start()

    def both(k):
        if k >= groups:
            return

        def one(g, carry):
            encode(k, g)
            return carry

        lax.fori_loop(0, blocks, one, 0)

    third = 2 if final > 2 else final + 1
    steps = {
        0: lambda: forward(0, 0),
        3: lambda: final > 1 and forward(0, 1),
        5: lambda: forward(1, 0),
        8: lambda: (final > 1 and forward(1, 1), final > 2 and begin(2)),
        9: lambda: (accept(0, 0), accept(1, 0)),
        10: lambda: final > 1 and (accept(0, 1), accept(1, 1)),
        12: lambda: (forward(0, third), rest(0)),
        13: lambda: final > 1 and rest(1),
        14: lambda: (ready(0), encode(0, 0)),
        15: lambda: (forward(1, third), spread_out()),
    }
    count_of = len(fine)
    for p, (i, start, count) in enumerate(fine):
        wait_for(ns, 0, (i, start, count))
        rows = pl.ds(start, count)
        gath[i, pl.ds(pl.multiple_of(t * slices + start, 16), count), :] = current(ns, 0, i, rows)
        for j in range(1, nt):
            y_copy(i, start, count, j).start()
        for at in range(2 * CAP):
            if max((at + 1) * count_of // (2 * CAP) - 1, 0) == p and at in steps:
                steps[at]()
        if start + count == slices and i >= 2:
            normalize(i - 2)

    ready(1)
    encode(1, 0)
    normalize(CAP - 2)
    accept(0, third)
    ready(2)
    encode(2, 0)
    normalize(CAP - 1)
    encode(0, 1)
    accept(1, third)
    forward(0, final)
    encode(1, 1)
    encode(2, 1)
    rest(third)
    later = range(3, groups)
    for k in later:
        ready(k)
        if k < groups - 1:
            both(k)
    forward(1, final)
    accept(0, final)
    accept(1, final)
    if later:
        encode(later[-1], 0)
    rest(final)
    if later:
        encode(later[-1], 1)

    def partial(source, cols):
        weight = wo[source].reshape(slices, slices)
        block = ctx[pl.ds(pl.multiple_of(source * slices, 16), slices), cols]
        return jnp.dot(weight, block, preferred_element_type=jnp.float32).astype(own.dtype)

    for j in range(1, nt):
        at = gath.at[:, pl.ds(0, slices), :]
        remote(at, at, y_send.at[j - 1], y_recv.at[0, j - 1], tensor=(t + j) % nt).wait_send()
    for s in range(ns):
        for slot in range(nb >> (s + 1)):
            remote(
                sends[s].at[slot], recvs[s].at[slot], t_send.at[s, slot], t_recv[s].at[slot, 0],
                bal=flip(b, bits[s]),
            ).wait_send()

    @pl.when(keeper != t)
    def _():
        cross(t, keeper).wait_send()

    def drain_line(s, carry):
        for way in range(2):
            step = 1 - 2 * way
            src = z - step * s
            there = z + step
            goes = (there >= 0) & (there < nd)
            at = wq.at[:, jnp.clip(src, 0, nd - 1), part]
            copy = remote(
                at, at, l_send.at[way, s, 0], l_recv.at[way, s, 0], dp=jnp.clip(there, 0, nd - 1)
            )
            pl.when(exists(src, 0) & goes)(copy.wait_send)
            valid, copy = line(way, s, final)
            pl.when(valid)(copy.wait_send)
        return carry

    lax.fori_loop(0, nd - 1, drain_line, 0)
    if part_count > 1:
        at = wq.at[:, pl.ds(0, nd - 1), part]
        remote(at, at, h_send.at[0], h_recv.at[0], bal=flip(b, 1)).wait_send()

    for s in range(1, ns + 1):
        finish(s)

    def mine(n, carry):
        own[:, columns(PAIR * n, PAIR)] = partial(t, columns(PAIR * n, PAIR))
        return carry

    lax.fori_loop(0, CAP // PAIR, mine, 0)

    def close(n, carry):
        i = n * PAIR
        for j in range(1, nt):
            at = ctx.at[pl.ds(0, slices), columns(i, PAIR)]
            arrived = remote(at, at, c_send.at[j - 1], c_recv.at[n, j - 1], tensor=(t + j) % nt)
            arrived.wait_recv()
        total = own[:, columns(i, PAIR)].astype(jnp.float32)
        for j in range(1, nt):
            total = total + partial((t + j) % nt, columns(i, PAIR)).astype(jnp.float32)
        for e in range(PAIR):
            source = gath[i + e, pl.ds(pl.multiple_of(t * slices, 16), slices), :]
            out[i + e] = (
                source.astype(jnp.float32) + total[:, e * patches : (e + 1) * patches]
            ).astype(out.dtype)
        return carry

    lax.fori_loop(0, CAP // PAIR, close, 0)
    for j in range(1, nt):
        at = ctx.at[pl.ds(0, slices), :]
        remote(at, at, c_send.at[j - 1], c_recv.at[0, j - 1], tensor=(t + j) % nt).wait_send()
    at = wo.at[:, :, pl.ds(0, nb - 1)]
    remote(at, at, d_send.at[0], d_recv.at[0], bal=flip(b, 1)).wait_send()


def encode_all(counts, ordering, tiles, qkv_weight, out_weight):
    nd, nb, nt = (lax.axis_size(name) for name in ("dp", "bal", "tensor"))
    ns = len(bits_of(nb))
    slots, slices, patches = tiles.shape
    kinds, rows, columns = qkv_weight.shape
    width, groups = column_groups(columns)
    waves = len(waves_of(groups))
    per = nd // nt
    wq = qkv_weight.reshape(kinds, min(nb, 2), -1, columns)
    wo = out_weight.reshape(nb, -1, columns)
    dtype = tiles.dtype
    vmem = pl.BlockSpec(memory_space=pltpu.VMEM)
    hbm = pl.BlockSpec(memory_space=pltpu.HBM)
    dma = pltpu.SemaphoreType.DMA

    def space(*shape):
        return pltpu.VMEM(shape, dtype)

    buffers = [space(nb >> (s + 1), CAP, slices, patches) for s in range(ns)]
    return pl.pallas_call(
        functools.partial(encode_kernel, (nd, nb, nt)),
        out_shape=jax.ShapeDtypeStruct((CAP, slices, patches), dtype),
        in_specs=[hbm] * 5,
        out_specs=vmem,
        scratch_shapes=buffers
        + buffers
        + [
            space(slots, slices, patches),
            space(CAP, nt * slices, patches),
            space(kinds, nd, *wq.shape[1:]),
            space(groups, kinds * width, nt * slices),
            space(*wo.shape),
            space(nt, per, *wo.shape),
            space(nt * slices, CAP * patches),
            space(kinds, columns, CAP * patches),
            space(nt * slices, CAP * patches),
            space(slices, CAP * patches),
        ]
        + [pltpu.SMEM(counts.shape, counts.dtype), pltpu.SMEM(ordering.shape, ordering.dtype)]
        + [
            dma((nb >> (s + 1), len(pieces_of(slices, QUARTERS if s == ns - 1 else 1))))
            for s in range(ns)
        ]
        + [dma((ns, max(nb // 2, 1))), dma((nt - 1,)), dma((CAP, nt - 1))]
        + [dma((nt - 1,)), dma((CAP // PAIR, nt - 1))]
        + [dma((2, nd - 1, 2)), dma((2, nd - 1, waves + 1)), dma((1,)), dma((waves,))]
        + [dma((1,)), dma((nt,)), dma((1,)), dma((per,)), dma((ns,)), dma((5,))],
        compiler_params=pltpu.CompilerParams(
            collective_id=0, has_side_effects=True, vmem_limit_bytes=44 * 1024 * 1024
        ),
        name="encode_all",
    )(*(pltpu.with_memory_space_constraint(a, pltpu.HBM) for a in (counts, ordering, tiles, wq, wo)))


def local(tiles, tile_counts, doc_order, qkv_weight, out_weight):
    own_tiles = tiles[0, 0]
    return encode_all(tile_counts, doc_order, own_tiles, qkv_weight, out_weight)[None]


def solution(mesh):
    placed = (
        P("dp", "bal", None, "tensor", None),
        P("dp", None),
        P("dp", None),
        P(None, "dp", "tensor"),
        P("dp", "tensor"),
    )
    return jax.shard_map(
        local, mesh=mesh, in_specs=placed, out_specs=P("dp", "bal", "tensor", None), check_vma=False
    )
```

```python
import functools

import jax
import jax.numpy as jnp
from jax import lax
from jax.experimental import pallas as pl
from jax.experimental.pallas import tpu as pltpu
from jax.sharding import PartitionSpec as P

HDIM = 80
CAP = 8
LANES = 128
GROUP = 4
PAIR = 2
QUARTERS = 4
EPSILON = 1e-06
LOG2E = 1.4426950408889634
MESH = pl.DeviceIdType.MESH


def flip(index, bit):
    return index + bit - 2 * bit * ((index // bit) % 2)


def bits_of(size):
    bits = []
    while 1 << len(bits) < size:
        bits.append(1 << len(bits))
    return bits


def column_groups(slices):
    width = LANES if slices % LANES == 0 else slices
    return width, slices // width


def pieces_of(slices, parts):
    part = slices // parts if slices % (16 * parts) == 0 else slices
    return [(i, start, part) for i in range(CAP) for start in range(0, slices, part)]


def step_pieces(slices, last):
    fine = pieces_of(slices, QUARTERS)
    if last:
        return fine
    lead = fine[0][2]
    first = [(0, 0, lead)] + ([(0, lead, slices - lead)] if lead < slices else [])
    return first + [(i, 0, slices) for i in range(1, CAP)]


def waves_of(groups):
    waves, start = [], 0
    for count in (1, 2, 1):
        if start + count < groups:
            waves.append((start, count))
            start += count
    return waves + [(start, groups - start)]


def remote(src, dst, send, recv, **device):
    return pltpu.make_async_remote_copy(
        src_ref=src, dst_ref=dst, send_sem=send, recv_sem=recv, device_id=device, device_id_type=MESH
    )


def encode_kernel(sizes, *refs):
    nd, nb, nt = sizes
    bits = bits_of(nb)
    ns = len(bits)
    counts_in, order_in, tiles_in, wq_in, wo_in, out = refs[:6]
    sends, recvs = refs[6 : 6 + ns], refs[6 + ns : 6 + 2 * ns]
    head, tail, gath, wq, wt, wo_own, wo, normed, qkv, ctx, own, counts, order = refs[
        6 + 2 * ns : 19 + 2 * ns
    ]
    t_recv = refs[19 + 2 * ns : 19 + 3 * ns]
    t_send, y_send, y_recv, c_send, c_recv, l_send, l_recv, h_send, h_recv = refs[
        19 + 3 * ns : 28 + 3 * ns
    ]
    x_send, x_recv, d_send, d_recv, e_recv, i_sem = refs[28 + 3 * ns :]
    z, b, t = lax.axis_index("dp"), lax.axis_index("bal"), lax.axis_index("tensor")
    slots, slices, patches = tiles_in.shape
    lead = head.shape[1]
    width, groups = column_groups(slices)
    waves = waves_of(groups)
    final = len(waves)
    pieces = [step_pieces(slices, s == ns - 1) for s in range(ns)]
    per = nd // nt
    features = nt * slices
    kinds = wq.shape[0]
    blocks = CAP // GROUP

    barrier = pltpu.get_barrier_semaphore()
    for m in bits:
        pl.semaphore_signal(barrier, inc=1, device_id={"bal": flip(b, m)}, device_id_type=MESH)
    for j in range(1, nt):
        pl.semaphore_signal(barrier, inc=1, device_id={"tensor": (t + j) % nt}, device_id_type=MESH)

    for step in (-1, 1):

        @pl.when((z + step >= 0) & (z + step < nd))
        def _(step=step):
            there = jnp.clip(z + step, 0, nd - 1)
            pl.semaphore_signal(barrier, inc=1, device_id={"dp": there}, device_id_type=MESH)

    greeted = jnp.int32(z > 0) + jnp.int32(z < nd - 1)

    load_counts = pltpu.make_async_copy(counts_in, counts, i_sem.at[3])
    load_order = pltpu.make_async_copy(order_in, order, i_sem.at[4])
    load_head = pltpu.make_async_copy(tiles_in.at[:, pl.ds(0, lead)], head, i_sem.at[0])
    load_tail = pltpu.make_async_copy(
        tiles_in.at[:, pl.ds(lead, slices - lead)], tail, i_sem.at[5]
    )
    load_q = pltpu.make_async_copy(wq_in, wq.at[:, z], i_sem.at[1])
    load_o = pltpu.make_async_copy(wo_in, wo_own, i_sem.at[2])
    load_counts.start()
    load_order.start()
    load_head.start()
    load_tail.start()
    load_q.start()
    load_o.start()
    load_counts.wait()
    load_order.wait()

    docs = order.shape[1]
    placed = [order[0, p] for p in range(docs)]
    edges = [jnp.int32(0)]
    for doc in placed:
        edges.append(edges[-1] + counts[0, doc])
    own_start = jnp.int32(0)
    for p in range(docs):
        own_start = own_start + jnp.where(placed[p] == b, edges[p], 0)

    def slot_of(s, r):
        return r >> (s + 1)

    def current(s, r, i, start, count):
        rows = pl.ds(start, count)
        block = b
        for m in bits:
            if r & m:
                block = flip(block, m)
        packed = block * CAP + i
        owner = jnp.int32(0)
        for p in range(docs):
            inside = (edges[p] <= packed) & (packed < edges[p + 1])
            owner = owner + jnp.where(inside, placed[p], 0)
        at = jnp.clip(packed - own_start, 0, slots - 1)
        value = head[at] if start == 0 else tail[at, pl.ds(start - lead, count)]
        for q in range(s):
            apart = (owner // bits[q]) % 2 != (b // bits[q]) % 2
            value = lax.select(apart, recvs[q][slot_of(q, r), i, rows], value)
        return value

    def tile_copy(s, slot, p):
        i, start, count = pieces[s][p]
        rows = pl.ds(start, count)
        return remote(
            sends[s].at[slot, i, rows],
            recvs[s].at[slot, i, rows],
            t_send.at[s, slot],
            t_recv[s].at[slot, p],
            bal=flip(b, bits[s]),
        )

    def wait_for(s, r, piece):
        i, start, count = piece
        for q in range(s):
            for p, (tile, first, number) in enumerate(pieces[q]):
                if tile == i and start <= first < start + count:
                    tile_copy(q, slot_of(q, r), p).wait_recv()

    def wanted(s):
        m = bits[s]
        return [r for r in reversed(range(nb)) if r & (m - 1) == 0 and r & m]

    load_head.wait()
    for r in wanted(0):
        sends[0][slot_of(0, r - 1), 0, pl.ds(0, lead)] = current(0, r, 0, 0, lead)
    pl.semaphore_wait(barrier, ns + nt - 1 + greeted)
    for r in wanted(0):
        tile_copy(0, slot_of(0, r - 1), 0).start()
    load_tail.wait()
    for r in wanted(0):
        slot = slot_of(0, r - 1)
        sends[0][slot, 0, pl.ds(lead, slices - lead)] = current(0, r, 0, lead, slices - lead)
        tile_copy(0, slot, 1).start()

        def fill(i, carry, r=r, slot=slot):
            sends[0][slot, i, pl.ds(0, lead)] = current(0, r, i, 0, lead)
            sends[0][slot, i, pl.ds(lead, slices - lead)] = current(0, r, i, lead, slices - lead)
            return carry

        lax.fori_loop(1, CAP, fill, 0)
        for p in range(2, len(pieces[0])):
            tile_copy(0, slot, p).start()

    load_o.wait()
    load_q.wait()
    keeper = z // per
    place = z % per

    @pl.when(keeper == t)
    def _():
        wo[t, place, b] = wo_own[b]

    part_count = wq.shape[2]
    part = b % part_count

    def held(src, w):
        src = jnp.clip(src, 0, nd - 1)
        if w == final:
            return wo.at[:, src % per, b]
        start, count = waves[w]
        return wq.at[:, src, part, :, pl.ds(start * width, count * width)]

    def exists(src, w):
        valid = (src >= 0) & (src < nd)
        return valid & (src // per == t) if w == final else valid

    def line(way, s, w):
        step = 1 - 2 * way
        src = z - step * s
        there = z + step
        at = held(src, w)
        at_step = min(s, nd - 2) if isinstance(s, int) else jnp.minimum(s, nd - 2)
        copy = remote(
            at, at, l_send.at[way, at_step, int(w == final)], l_recv.at[way, at_step, w],
            dp=jnp.clip(there, 0, nd - 1),
        )
        return exists(src, w) & (there >= 0) & (there < nd), copy

    def doubled(q, s, e):
        at = b
        for bit in range(s):
            if (e >> bit) & 1:
                at = flip(at, bits[ns - 1 - bit])
        rows = wo.at[:, q, at]
        landed = e_recv.at[s, q] if s else d_recv.at[q]
        return remote(rows, rows, d_send.at[0], landed, bal=flip(b, bits[ns - 1 - s]))

    def arrival(way, s, w):
        step = 1 - 2 * way
        src = z - step * (s + 1)
        at = held(src, w)
        here = remote(
            at, at, l_send.at[way, s, 0], l_recv.at[way, s, w], dp=jnp.clip(z + step, 0, nd - 1)
        )
        if w == final:
            return exists(src, w), here, doubled(jnp.clip(src, 0, nd - 1) % per, 0, 0)
        return exists(src, w), here, remote(at, at, h_send.at[0], h_recv.at[w], bal=flip(b, 1))

    def begin(w):
        for way in range(2):
            valid, copy = line(way, 0, w)
            pl.when(valid)(copy.start)

    early = min(2, nd - 1)

    def hop(s, w, onward):
        for way in range(2):
            valid, here, half = arrival(way, s, w)
            further, copy = line(way, s + 1, w)

            @pl.when(valid & (further if onward else jnp.logical_not(further)))
            def _(here=here, half=half, copy=copy):
                here.wait_recv()
                if onward:
                    copy.start()
                if part_count > 1 or w == final:
                    half.start()

    def forward(s, w):
        if s < early and w <= final:
            hop(s, w, True)

    def accept(s, w):
        if s < early and w <= final:
            hop(s, w, False)

    def rest(w):
        def one(s, carry):
            hop(s, w, True)
            hop(s, w, False)
            return carry

        if w <= final:
            lax.fori_loop(early, nd - 1, one, 0)

    for w in range(min(2, final)):
        begin(w)

    def cross(source, target):
        return remote(
            wo_own.at[b], wo.at[source, place, b], x_send.at[0], x_recv.at[source], tensor=target
        )

    @pl.when(keeper != t)
    def _():
        cross(t, keeper).start()

    def spread_out():
        @pl.when(keeper == t)
        def _():
            for j in range(1, nt):
                cross((t + j) % nt, t).wait_recv()
            begin(final)
            doubled(place, 0, 0).start()

    def source_of(i):
        low = t * per
        near = jnp.where(z < low, i, per - 1 - i)
        return jnp.where((z >= low) & (z < low + per), (place + i) % per, near)

    def complete(q):
        doubled(q, 0, 0).wait_recv()
        for s in range(1, ns):
            for e in range(1 << s):
                doubled(q, s, e).start()
            at = wo.at[:, q, pl.ds(0, 1 << s)]
            remote(at, at, d_send.at[0], e_recv.at[s, q], bal=flip(b, bits[ns - 1 - s])).wait_recv()

    for s in range(1, ns):
        for r in wanted(s):
            slot = slot_of(s, r - bits[s])
            for p, (i, start, count) in enumerate(pieces[s]):
                wait_for(s, r, pieces[s][p])
                rows = pl.ds(start, count)
                sends[s][slot, i, rows] = current(s, r, i, start, count)
                tile_copy(s, slot, p).start()

    fine = pieces[ns - 1]

    def y_copy(i, start, count, j):
        at = gath.at[i, pl.ds(pl.multiple_of(t * slices + start, 16), count), :]
        return remote(at, at, y_send.at[j - 1], y_recv.at[i, j - 1], tensor=(t + j) % nt)

    def normalize(i):
        for j in range(1, nt):
            y_copy(i, 0, slices, j).wait_recv()
        values = gath[i].astype(jnp.float32)
        center = values - jnp.mean(values, axis=0, keepdims=True)
        spread_of = jnp.mean(center * center, axis=0, keepdims=True)
        normed[:, i * patches : (i + 1) * patches] = (
            center * lax.rsqrt(spread_of + EPSILON)
        ).astype(normed.dtype)

    def ready(k):
        if k >= groups:
            return

        for w, (start, count) in enumerate(waves):
            if part_count > 1 and start == k:
                at = wq.at[:, pl.ds(0, nd - 1), part, :, pl.ds(start * width, count * width)]
                remote(at, at, h_send.at[0], h_recv.at[w], bal=flip(b, 1)).wait_recv()
        for kind in range(kinds):
            block = wq[kind, :, :, :, k * width : (k + 1) * width].reshape(features, width)
            wt[k, kind * width : (kind + 1) * width, :] = block.T

    def heads_of(k):
        return [h for h in range(slices // HDIM) if k * width < (h + 1) * HDIM <= (k + 1) * width]

    def c_copy(k, n, j):
        first, number = heads_of(k)[0], len(heads_of(k))
        at = ctx.at[
            pl.ds(pl.multiple_of(t * slices + first * HDIM, 16), number * HDIM),
            pl.ds(pl.multiple_of(n * PAIR * patches, patches), PAIR * patches),
        ]
        return remote(at, at, c_send.at[j - 1], c_recv.at[n, j - 1], tensor=(t + j) % nt)

    def columns(i, number):
        return pl.ds(pl.multiple_of(i * patches, patches), number * patches)

    scale = HDIM ** (-0.5) * LOG2E

    def encode(k, g):
        if k >= groups:
            return
        for n in range(0, GROUP, PAIR):
            cols = columns(g * GROUP + n, PAIR)
            result = jnp.dot(wt[k], normed[:, cols], preferred_element_type=jnp.float32)
            for kind in range(kinds):
                qkv[kind, k * width : (k + 1) * width, cols] = result[
                    kind * width : (kind + 1) * width
                ].astype(qkv.dtype)
        for n in range(GROUP):
            cols = columns(g * GROUP + n, 1)
            for h in heads_of(k):
                span = slice(h * HDIM, (h + 1) * HDIM)
                scores = lax.dot_general(
                    qkv[1, span, cols], qkv[0, span, cols], (((0,), (0,)), ((), ())),
                    preferred_element_type=jnp.float32,
                )
                powers = jnp.exp2((scores - jnp.max(scores, axis=0, keepdims=True)) * scale)
                total = jnp.sum(powers, axis=0, keepdims=True)
                value = jnp.dot(
                    qkv[2, span, cols], powers.astype(qkv.dtype), preferred_element_type=jnp.float32
                )
                ctx[pl.ds(pl.multiple_of(t * slices + h * HDIM, 16), HDIM), cols] = (
                    value * (1.0 / total)
                ).astype(ctx.dtype)
        for n in range(GROUP // PAIR):
            for j in range(1, nt):
                c_copy(k, g * (GROUP // PAIR) + n, j).start()

    third = 2 if final > 2 else final + 1
    fourth = 3 if final > 3 else final + 1
    steps = {
        0: lambda: forward(0, 0),
        3: lambda: final > 1 and forward(0, 1),
        5: lambda: forward(1, 0),
        8: lambda: (final > 1 and forward(1, 1), final > 2 and begin(2), final > 3 and begin(3)),
        9: lambda: (accept(0, 0), accept(1, 0)),
        10: lambda: final > 1 and (accept(0, 1), accept(1, 1)),
        11: lambda: forward(0, third),
        12: lambda: (forward(0, fourth), rest(0)),
        13: lambda: final > 1 and rest(1),
        14: lambda: (forward(1, third), ready(0), encode(0, 0)),
        15: lambda: (forward(1, fourth), spread_out()),
    }
    count_of = len(fine)
    for p, (i, start, count) in enumerate(fine):
        wait_for(ns, 0, (i, start, count))
        gath[i, pl.ds(pl.multiple_of(t * slices + start, 16), count), :] = current(
            ns, 0, i, start, count
        )
        for j in range(1, nt):
            y_copy(i, start, count, j).start()
        for at in range(2 * CAP):
            if max((at + 1) * count_of // (2 * CAP) - 1, 0) == p and at in steps:
                steps[at]()
        if start + count == slices and i >= 2:
            normalize(i - 2)

    ready(1)
    encode(1, 0)
    normalize(CAP - 2)
    accept(0, third)
    accept(0, fourth)
    ready(2)
    encode(2, 0)
    normalize(CAP - 1)
    encode(0, 1)
    accept(1, third)
    accept(1, fourth)
    forward(0, final)
    encode(1, 1)
    rest(third)
    encode(2, 1)
    later = range(3, groups)
    for k in later[:-1]:
        ready(k)
        encode(k, 0)
        if k == 3:
            rest(fourth)
        encode(k, 1)
    if len(later) == 1:
        rest(fourth)
    for k in later[-1:]:
        ready(k)
    forward(1, final)
    accept(0, final)
    accept(1, final)
    if later:
        encode(later[-1], 0)
    rest(final)
    if later:
        encode(later[-1], 1)

    def partial(source, cols):
        weight = wo[source].reshape(slices, slices)
        block = ctx[pl.ds(pl.multiple_of(source * slices, 16), slices), cols]
        return jnp.dot(weight, block, preferred_element_type=jnp.float32).astype(own.dtype)

    for j in range(1, nt):
        at = gath.at[:, pl.ds(0, slices), :]
        remote(at, at, y_send.at[j - 1], y_recv.at[0, j - 1], tensor=(t + j) % nt).wait_send()
    for s in range(ns):
        for slot in range(nb >> (s + 1)):
            remote(
                sends[s].at[slot], recvs[s].at[slot], t_send.at[s, slot], t_recv[s].at[slot, 0],
                bal=flip(b, bits[s]),
            ).wait_send()

    @pl.when(keeper != t)
    def _():
        cross(t, keeper).wait_send()

    def drain_line(s, carry):
        for way in range(2):
            step = 1 - 2 * way
            src = z - step * s
            there = z + step
            goes = (there >= 0) & (there < nd)
            at = wq.at[:, jnp.clip(src, 0, nd - 1), part]
            copy = remote(
                at, at, l_send.at[way, s, 0], l_recv.at[way, s, 0], dp=jnp.clip(there, 0, nd - 1)
            )
            pl.when(exists(src, 0) & goes)(copy.wait_send)
            valid, copy = line(way, s, final)
            pl.when(valid)(copy.wait_send)
        return carry

    lax.fori_loop(0, nd - 1, drain_line, 0)
    if part_count > 1:
        at = wq.at[:, pl.ds(0, nd - 1), part]
        remote(at, at, h_send.at[0], h_recv.at[0], bal=flip(b, 1)).wait_send()

    part_rows = slices // per

    def mine(i, carry):
        q = source_of(i)
        complete(q)
        weight = wo[t, q].reshape(part_rows, slices)

        def one(n, carry):
            block = ctx[pl.ds(pl.multiple_of(t * slices, 16), slices), columns(n * PAIR, PAIR)]
            own[q, :, columns(n * PAIR, PAIR)] = jnp.dot(
                weight, block, preferred_element_type=jnp.float32
            ).astype(own.dtype)
            return carry

        lax.fori_loop(0, CAP // PAIR, one, 0)
        return carry

    lax.fori_loop(0, per, mine, 0)

    def close(n, carry):
        i = n * PAIR
        for j in range(1, nt):
            at = ctx.at[pl.ds(0, slices), columns(i, PAIR)]
            arrived = remote(at, at, c_send.at[j - 1], c_recv.at[n, j - 1], tensor=(t + j) % nt)
            arrived.wait_recv()
        total = own[:, :, columns(i, PAIR)].reshape(slices, PAIR * patches).astype(jnp.float32)
        for j in range(1, nt):
            total = total + partial((t + j) % nt, columns(i, PAIR)).astype(jnp.float32)
        for e in range(PAIR):
            source = gath[i + e, pl.ds(pl.multiple_of(t * slices, 16), slices), :]
            out[i + e] = (
                source.astype(jnp.float32) + total[:, e * patches : (e + 1) * patches]
            ).astype(out.dtype)
        return carry

    lax.fori_loop(0, CAP // PAIR, close, 0)
    for j in range(1, nt):
        at = ctx.at[pl.ds(0, slices), :]
        remote(at, at, c_send.at[j - 1], c_recv.at[0, j - 1], tensor=(t + j) % nt).wait_send()
    at = wo.at[:, :, pl.ds(0, nb - 1)]
    remote(at, at, d_send.at[0], d_recv.at[0], bal=flip(b, 1)).wait_send()


def encode_all(counts, ordering, tiles, qkv_weight, out_weight):
    nd, nb, nt = (lax.axis_size(name) for name in ("dp", "bal", "tensor"))
    ns = len(bits_of(nb))
    slots, slices, patches = tiles.shape
    kinds, rows, columns = qkv_weight.shape
    width, groups = column_groups(columns)
    waves = len(waves_of(groups))
    lead = pieces_of(slices, QUARTERS)[0][2]
    per = nd // nt
    wq = qkv_weight.reshape(kinds, min(nb, 2), -1, columns)
    wo = out_weight.reshape(nb, -1, columns)
    dtype = tiles.dtype
    vmem = pl.BlockSpec(memory_space=pltpu.VMEM)
    hbm = pl.BlockSpec(memory_space=pltpu.HBM)
    dma = pltpu.SemaphoreType.DMA

    def space(*shape):
        return pltpu.VMEM(shape, dtype)

    buffers = [space(nb >> (s + 1), CAP, slices, patches) for s in range(ns)]
    return pl.pallas_call(
        functools.partial(encode_kernel, (nd, nb, nt)),
        out_shape=jax.ShapeDtypeStruct((CAP, slices, patches), dtype),
        in_specs=[hbm] * 5,
        out_specs=vmem,
        scratch_shapes=buffers
        + buffers
        + [
            space(slots, lead, patches),
            space(slots, slices - lead, patches),
            space(CAP, nt * slices, patches),
            space(kinds, nd, *wq.shape[1:]),
            space(groups, kinds * width, nt * slices),
            space(*wo.shape),
            space(nt, per, *wo.shape),
            space(nt * slices, CAP * patches),
            space(kinds, columns, CAP * patches),
            space(nt * slices, CAP * patches),
            space(per, slices // per, CAP * patches),
        ]
        + [pltpu.SMEM(counts.shape, counts.dtype), pltpu.SMEM(ordering.shape, ordering.dtype)]
        + [
            dma((nb >> (s + 1), len(step_pieces(slices, s == ns - 1))))
            for s in range(ns)
        ]
        + [dma((ns, max(nb // 2, 1))), dma((nt - 1,)), dma((CAP, nt - 1))]
        + [dma((nt - 1,)), dma((CAP // PAIR, nt - 1))]
        + [dma((2, nd - 1, 2)), dma((2, nd - 1, waves + 1)), dma((1,)), dma((waves,))]
        + [dma((1,)), dma((nt,)), dma((1,)), dma((per,)), dma((ns, per)), dma((6,))],
        compiler_params=pltpu.CompilerParams(
            collective_id=0, has_side_effects=True, vmem_limit_bytes=44 * 1024 * 1024
        ),
        name="encode_all",
    )(*(pltpu.with_memory_space_constraint(a, pltpu.HBM) for a in (counts, ordering, tiles, wq, wo)))


def local(tiles, tile_counts, doc_order, qkv_weight, out_weight):
    own_tiles = tiles[0, 0]
    return encode_all(tile_counts, doc_order, own_tiles, qkv_weight, out_weight)[None]


def solution(mesh):
    placed = (
        P("dp", "bal", None, "tensor", None),
        P("dp", None),
        P("dp", None),
        P(None, "dp", "tensor"),
        P("dp", "tensor"),
    )
    return jax.shard_map(
        local, mesh=mesh, in_specs=placed, out_specs=P("dp", "bal", "tensor", None), check_vma=False
    )
```

```python
import functools

import jax
import jax.numpy as jnp
from jax import lax
from jax.experimental import pallas as pl
from jax.experimental.pallas import tpu as pltpu
from jax.sharding import PartitionSpec as P

HDIM = 80
CAP = 8
LANES = 128
GROUP = 4
PAIR = 2
QUARTERS = 4
EPSILON = 1e-06
LOG2E = 1.4426950408889634
MESH = pl.DeviceIdType.MESH


def flip(index, bit):
    return index + bit - 2 * bit * ((index // bit) % 2)


def bits_of(size):
    bits = []
    while 1 << len(bits) < size:
        bits.append(1 << len(bits))
    return bits


def column_groups(slices):
    width = LANES if slices % LANES == 0 else slices
    return width, slices // width


def pieces_of(slices, parts):
    part = slices // parts if slices % (16 * parts) == 0 else slices
    return [(i, start, part) for i in range(CAP) for start in range(0, slices, part)]


def step_pieces(slices, last):
    fine = pieces_of(slices, QUARTERS)
    if last:
        return fine
    lead = fine[0][2]
    first = [(0, 0, lead)] + ([(0, lead, slices - lead)] if lead < slices else [])
    return first + [(i, 0, slices) for i in range(1, CAP)]


def waves_of(groups):
    waves, start = [], 0
    for count in (1, 2, 1):
        if start + count < groups:
            waves.append((start, count))
            start += count
    return waves + [(start, groups - start)]


def remote(src, dst, send, recv, **device):
    return pltpu.make_async_remote_copy(
        src_ref=src, dst_ref=dst, send_sem=send, recv_sem=recv, device_id=device, device_id_type=MESH
    )


def encode_kernel(sizes, *refs):
    nd, nb, nt = sizes
    bits = bits_of(nb)
    ns = len(bits)
    counts_in, order_in, tiles_in, wq_in, wo_in, out = refs[:6]
    sends, recvs = refs[6 : 6 + ns], refs[6 + ns : 6 + 2 * ns]
    head, tail, gath, wq, wt, wo_own, wo, normed, qkv, ctx, own, counts, order = refs[
        6 + 2 * ns : 19 + 2 * ns
    ]
    t_recv = refs[19 + 2 * ns : 19 + 3 * ns]
    t_send, y_send, y_recv, c_send, c_recv, l_send, l_recv, h_send, h_recv = refs[
        19 + 3 * ns : 28 + 3 * ns
    ]
    x_send, x_recv, d_send, d_recv, e_recv, i_sem = refs[28 + 3 * ns :]
    z, b, t = lax.axis_index("dp"), lax.axis_index("bal"), lax.axis_index("tensor")
    slots, slices, patches = tiles_in.shape
    lead = head.shape[1]
    width, groups = column_groups(slices)
    waves = waves_of(groups)
    final = len(waves)
    pieces = [step_pieces(slices, s == ns - 1) for s in range(ns)]
    per = nd // nt
    features = nt * slices
    kinds = wq.shape[0]
    blocks = CAP // GROUP

    barrier = pltpu.get_barrier_semaphore()
    for m in bits:
        pl.semaphore_signal(barrier, inc=1, device_id={"bal": flip(b, m)}, device_id_type=MESH)
    for j in range(1, nt):
        pl.semaphore_signal(barrier, inc=1, device_id={"tensor": (t + j) % nt}, device_id_type=MESH)

    for step in (-1, 1):

        @pl.when((z + step >= 0) & (z + step < nd))
        def _(step=step):
            there = jnp.clip(z + step, 0, nd - 1)
            pl.semaphore_signal(barrier, inc=1, device_id={"dp": there}, device_id_type=MESH)

    greeted = jnp.int32(z > 0) + jnp.int32(z < nd - 1)

    load_counts = pltpu.make_async_copy(counts_in, counts, i_sem.at[3])
    load_order = pltpu.make_async_copy(order_in, order, i_sem.at[4])
    load_head = pltpu.make_async_copy(tiles_in.at[:, pl.ds(0, lead)], head, i_sem.at[0])
    load_tail = pltpu.make_async_copy(
        tiles_in.at[:, pl.ds(lead, slices - lead)], tail, i_sem.at[5]
    )
    load_q = pltpu.make_async_copy(wq_in, wq.at[:, z], i_sem.at[1])
    load_o = pltpu.make_async_copy(wo_in, wo_own, i_sem.at[2])
    load_counts.start()
    load_order.start()
    load_head.start()
    load_tail.start()
    load_q.start()
    load_o.start()
    load_counts.wait()
    load_order.wait()

    docs = order.shape[1]
    placed = [order[0, p] for p in range(docs)]
    edges = [jnp.int32(0)]
    for doc in placed:
        edges.append(edges[-1] + counts[0, doc])
    own_start = jnp.int32(0)
    for p in range(docs):
        own_start = own_start + jnp.where(placed[p] == b, edges[p], 0)

    def slot_of(s, r):
        return r >> (s + 1)

    def current(s, r, i, start, count):
        rows = pl.ds(start, count)
        block = b
        for m in bits:
            if r & m:
                block = flip(block, m)
        packed = block * CAP + i
        owner = jnp.int32(0)
        for p in range(docs):
            inside = (edges[p] <= packed) & (packed < edges[p + 1])
            owner = owner + jnp.where(inside, placed[p], 0)
        at = jnp.clip(packed - own_start, 0, slots - 1)
        value = head[at] if start == 0 else tail[at, pl.ds(start - lead, count)]
        for q in range(s):
            apart = (owner // bits[q]) % 2 != (b // bits[q]) % 2
            value = lax.select(apart, recvs[q][slot_of(q, r), i, rows], value)
        return value

    def tile_copy(s, slot, p):
        i, start, count = pieces[s][p]
        rows = pl.ds(start, count)
        return remote(
            sends[s].at[slot, i, rows],
            recvs[s].at[slot, i, rows],
            t_send.at[s, slot],
            t_recv[s].at[slot, p],
            bal=flip(b, bits[s]),
        )

    def wait_for(s, r, piece):
        i, start, count = piece
        for q in range(s):
            for p, (tile, first, number) in enumerate(pieces[q]):
                if tile == i and start <= first < start + count:
                    tile_copy(q, slot_of(q, r), p).wait_recv()

    def wanted(s):
        m = bits[s]
        return [r for r in reversed(range(nb)) if r & (m - 1) == 0 and r & m]

    load_head.wait()
    for r in wanted(0):
        sends[0][slot_of(0, r - 1), 0, pl.ds(0, lead)] = current(0, r, 0, 0, lead)
    pl.semaphore_wait(barrier, ns + nt - 1 + greeted)
    for r in wanted(0):
        tile_copy(0, slot_of(0, r - 1), 0).start()
    load_tail.wait()
    for r in wanted(0):
        slot = slot_of(0, r - 1)
        sends[0][slot, 0, pl.ds(lead, slices - lead)] = current(0, r, 0, lead, slices - lead)
        tile_copy(0, slot, 1).start()

        def fill(i, carry, r=r, slot=slot):
            sends[0][slot, i, pl.ds(0, lead)] = current(0, r, i, 0, lead)
            sends[0][slot, i, pl.ds(lead, slices - lead)] = current(0, r, i, lead, slices - lead)
            return carry

        lax.fori_loop(1, CAP, fill, 0)
        for p in range(2, len(pieces[0])):
            tile_copy(0, slot, p).start()

    load_o.wait()
    load_q.wait()
    keeper = z // per
    place = z % per

    @pl.when(keeper == t)
    def _():
        wo[t, place, b] = wo_own[b]

    part_count = wq.shape[2]
    part = b % part_count

    def held(src, w):
        src = jnp.clip(src, 0, nd - 1)
        if w == final:
            return wo.at[:, src % per, b]
        start, count = waves[w]
        return wq.at[:, src, part, :, pl.ds(start * width, count * width)]

    def exists(src, w):
        valid = (src >= 0) & (src < nd)
        return valid & (src // per == t) if w == final else valid

    def line(way, s, w):
        step = 1 - 2 * way
        src = z - step * s
        there = z + step
        at = held(src, w)
        at_step = min(s, nd - 2) if isinstance(s, int) else jnp.minimum(s, nd - 2)
        copy = remote(
            at, at, l_send.at[way, at_step, int(w == final)], l_recv.at[jnp.clip(src, 0, nd - 1), w],
            dp=jnp.clip(there, 0, nd - 1),
        )
        return exists(src, w) & (there >= 0) & (there < nd), copy

    def doubled(q, s, e):
        at = b
        for bit in range(s):
            if (e >> bit) & 1:
                at = flip(at, bits[ns - 1 - bit])
        rows = wo.at[:, q, at]
        landed = e_recv.at[s - 1, q] if s else d_recv.at[q]
        return remote(rows, rows, d_send.at[0], landed, bal=flip(b, bits[ns - 1 - s]))

    def arrival(way, s, w):
        step = 1 - 2 * way
        src = z - step * (s + 1)
        at = held(src, w)
        here = remote(
            at, at, l_send.at[way, s, 0], l_recv.at[jnp.clip(src, 0, nd - 1), w],
            dp=jnp.clip(z + step, 0, nd - 1),
        )
        if w == final:
            return exists(src, w), here, doubled(jnp.clip(src, 0, nd - 1) % per, 0, 0)
        return exists(src, w), here, remote(at, at, h_send.at[0], h_recv.at[w], bal=flip(b, 1))

    def begin(w):
        for way in range(2):
            valid, copy = line(way, 0, w)
            pl.when(valid)(copy.start)

    early = min(2, nd - 1)

    def hop(s, w, onward):
        for way in range(2):
            valid, here, half = arrival(way, s, w)
            further, copy = line(way, s + 1, w)

            @pl.when(valid & (further if onward else jnp.logical_not(further)))
            def _(here=here, half=half, copy=copy):
                here.wait_recv()
                if onward:
                    copy.start()
                if part_count > 1 or w == final:
                    half.start()

    def forward(s, w):
        if s < early and w <= final:
            hop(s, w, True)

    def accept(s, w):
        if s < early and w <= final:
            hop(s, w, False)

    def rest(w):
        def one(s, carry):
            hop(s, w, True)
            hop(s, w, False)
            return carry

        if w <= final:
            lax.fori_loop(early, nd - 1, one, 0)

    for w in range(min(2, final)):
        begin(w)

    def cross(source, target):
        return remote(
            wo_own.at[b], wo.at[source, place, b], x_send.at[0], x_recv.at[source], tensor=target
        )

    @pl.when(keeper != t)
    def _():
        cross(t, keeper).start()

    def spread_out():
        @pl.when(keeper == t)
        def _():
            for j in range(1, nt):
                cross((t + j) % nt, t).wait_recv()
            begin(final)
            doubled(place, 0, 0).start()

    def source_of(i):
        low = t * per
        near = jnp.where(z < low, i, per - 1 - i)
        return jnp.where((z >= low) & (z < low + per), (place + i) % per, near)

    def complete(q):
        doubled(q, 0, 0).wait_recv()
        for s in range(1, ns):
            for e in range(1 << s):
                doubled(q, s, e).start()
            at = wo.at[:, q, pl.ds(0, 1 << s)]
            remote(at, at, d_send.at[0], e_recv.at[s - 1, q], bal=flip(b, bits[ns - 1 - s])).wait_recv()

    for s in range(1, ns):
        for r in wanted(s):
            slot = slot_of(s, r - bits[s])
            for p, (i, start, count) in enumerate(pieces[s]):
                wait_for(s, r, pieces[s][p])
                rows = pl.ds(start, count)
                sends[s][slot, i, rows] = current(s, r, i, start, count)
                tile_copy(s, slot, p).start()

    fine = pieces[ns - 1]

    def y_copy(i, start, count, j):
        at = gath.at[i, pl.ds(pl.multiple_of(t * slices + start, 16), count), :]
        return remote(at, at, y_send.at[j - 1], y_recv.at[i, j - 1], tensor=(t + j) % nt)

    def normalize(i):
        for j in range(1, nt):
            y_copy(i, 0, slices, j).wait_recv()
        values = gath[i].astype(jnp.float32)
        center = values - jnp.mean(values, axis=0, keepdims=True)
        spread_of = jnp.mean(center * center, axis=0, keepdims=True)
        normed[:, i * patches : (i + 1) * patches] = (
            center * lax.rsqrt(spread_of + EPSILON)
        ).astype(normed.dtype)

    def ready(k):
        if k >= groups:
            return

        for w, (start, count) in enumerate(waves):
            if part_count > 1 and start == k:
                at = wq.at[:, pl.ds(0, nd - 1), part, :, pl.ds(start * width, count * width)]
                remote(at, at, h_send.at[0], h_recv.at[w], bal=flip(b, 1)).wait_recv()
        for kind in range(kinds):
            block = wq[kind, :, :, :, k * width : (k + 1) * width].reshape(features, width)
            wt[k, kind * width : (kind + 1) * width, :] = block.T

    def heads_of(k):
        return [h for h in range(slices // HDIM) if k * width < (h + 1) * HDIM <= (k + 1) * width]

    def c_copy(k, n, j):
        first, number = heads_of(k)[0], len(heads_of(k))
        at = ctx.at[
            pl.ds(pl.multiple_of(t * slices + first * HDIM, 16), number * HDIM),
            pl.ds(pl.multiple_of(n * PAIR * patches, patches), PAIR * patches),
        ]
        return remote(at, at, c_send.at[j - 1], c_recv.at[n, j - 1], tensor=(t + j) % nt)

    def columns(i, number):
        return pl.ds(pl.multiple_of(i * patches, patches), number * patches)

    scale = HDIM ** (-0.5) * LOG2E

    def encode(k, g):
        if k >= groups:
            return
        for n in range(0, GROUP, PAIR):
            cols = columns(g * GROUP + n, PAIR)
            result = jnp.dot(wt[k], normed[:, cols], preferred_element_type=jnp.float32)
            for kind in range(kinds):
                qkv[kind, k * width : (k + 1) * width, cols] = result[
                    kind * width : (kind + 1) * width
                ].astype(qkv.dtype)
        for n in range(GROUP):
            cols = columns(g * GROUP + n, 1)
            for h in heads_of(k):
                span = slice(h * HDIM, (h + 1) * HDIM)
                scores = lax.dot_general(
                    qkv[1, span, cols], qkv[0, span, cols], (((0,), (0,)), ((), ())),
                    preferred_element_type=jnp.float32,
                )
                powers = jnp.exp2((scores - jnp.max(scores, axis=0, keepdims=True)) * scale)
                total = jnp.sum(powers, axis=0, keepdims=True)
                value = jnp.dot(
                    qkv[2, span, cols], powers.astype(qkv.dtype), preferred_element_type=jnp.float32
                )
                ctx[pl.ds(pl.multiple_of(t * slices + h * HDIM, 16), HDIM), cols] = (
                    value * (1.0 / total)
                ).astype(ctx.dtype)
        for n in range(GROUP // PAIR):
            for j in range(1, nt):
                c_copy(k, g * (GROUP // PAIR) + n, j).start()

    third = 2 if final > 2 else final + 1
    fourth = 3 if final > 3 else final + 1
    steps = {
        0: lambda: forward(0, 0),
        3: lambda: final > 1 and forward(0, 1),
        5: lambda: forward(1, 0),
        8: lambda: (final > 1 and forward(1, 1), final > 2 and begin(2), final > 3 and begin(3)),
        9: lambda: (accept(0, 0), accept(1, 0)),
        10: lambda: final > 1 and (accept(0, 1), accept(1, 1)),
        11: lambda: forward(0, third),
        12: lambda: (forward(0, fourth), rest(0)),
        13: lambda: final > 1 and rest(1),
        14: lambda: (forward(1, third), ready(0), encode(0, 0)),
        15: lambda: (forward(1, fourth), spread_out()),
    }
    count_of = len(fine)
    for p, (i, start, count) in enumerate(fine):
        wait_for(ns, 0, (i, start, count))
        gath[i, pl.ds(pl.multiple_of(t * slices + start, 16), count), :] = current(
            ns, 0, i, start, count
        )
        for j in range(1, nt):
            y_copy(i, start, count, j).start()
        for at in range(2 * CAP):
            if max((at + 1) * count_of // (2 * CAP) - 1, 0) == p and at in steps:
                steps[at]()
        if start + count == slices and i >= 2:
            normalize(i - 2)

    ready(1)
    encode(1, 0)
    normalize(CAP - 2)
    accept(0, third)
    accept(0, fourth)
    ready(2)
    encode(2, 0)
    normalize(CAP - 1)
    encode(0, 1)
    accept(1, third)
    accept(1, fourth)
    forward(0, final)
    encode(1, 1)
    rest(third)
    encode(2, 1)
    later = range(3, groups)
    for k in later[:-1]:
        ready(k)
        encode(k, 0)
        if k == 3:
            rest(fourth)
        encode(k, 1)
    if len(later) == 1:
        rest(fourth)
    for k in later[-1:]:
        ready(k)
    forward(1, final)
    accept(0, final)
    accept(1, final)
    if later:
        encode(later[-1], 0)
    rest(final)
    if later:
        encode(later[-1], 1)

    def partial(source, cols):
        weight = wo[source].reshape(slices, slices)
        block = ctx[pl.ds(pl.multiple_of(source * slices, 16), slices), cols]
        return jnp.dot(weight, block, preferred_element_type=jnp.float32).astype(own.dtype)

    for j in range(1, nt):
        at = gath.at[:, pl.ds(0, slices), :]
        remote(at, at, y_send.at[j - 1], y_recv.at[0, j - 1], tensor=(t + j) % nt).wait_send()
    for s in range(ns):
        for slot in range(nb >> (s + 1)):
            remote(
                sends[s].at[slot], recvs[s].at[slot], t_send.at[s, slot], t_recv[s].at[slot, 0],
                bal=flip(b, bits[s]),
            ).wait_send()

    @pl.when(keeper != t)
    def _():
        cross(t, keeper).wait_send()

    def drain_line(s, carry):
        for way in range(2):
            step = 1 - 2 * way
            src = z - step * s
            there = z + step
            goes = (there >= 0) & (there < nd)
            at = wq.at[:, jnp.clip(src, 0, nd - 1), part]
            copy = remote(
                at, at, l_send.at[way, s, 0], l_recv.at[0, 0], dp=jnp.clip(there, 0, nd - 1)
            )
            pl.when(exists(src, 0) & goes)(copy.wait_send)
            valid, copy = line(way, s, final)
            pl.when(valid)(copy.wait_send)
        return carry

    lax.fori_loop(0, nd - 1, drain_line, 0)
    if part_count > 1:
        at = wq.at[:, pl.ds(0, nd - 1), part]
        remote(at, at, h_send.at[0], h_recv.at[0], bal=flip(b, 1)).wait_send()

    part_rows = slices // per

    def mine(i, carry):
        q = source_of(i)
        complete(q)
        weight = wo[t, q].reshape(part_rows, slices)

        def one(n, carry):
            block = ctx[pl.ds(pl.multiple_of(t * slices, 16), slices), columns(n * PAIR, PAIR)]
            own[q, :, columns(n * PAIR, PAIR)] = jnp.dot(
                weight, block, preferred_element_type=jnp.float32
            ).astype(own.dtype)
            return carry

        lax.fori_loop(0, CAP // PAIR, one, 0)
        return carry

    lax.fori_loop(0, per, mine, 0)

    def close(n, carry):
        i = n * PAIR
        for j in range(1, nt):
            at = ctx.at[pl.ds(0, slices), columns(i, PAIR)]
            arrived = remote(at, at, c_send.at[j - 1], c_recv.at[n, j - 1], tensor=(t + j) % nt)
            arrived.wait_recv()
        total = own[:, :, columns(i, PAIR)].reshape(slices, PAIR * patches).astype(jnp.float32)
        for j in range(1, nt):
            total = total + partial((t + j) % nt, columns(i, PAIR)).astype(jnp.float32)
        for e in range(PAIR):
            source = gath[i + e, pl.ds(pl.multiple_of(t * slices, 16), slices), :]
            out[i + e] = (
                source.astype(jnp.float32) + total[:, e * patches : (e + 1) * patches]
            ).astype(out.dtype)
        return carry

    lax.fori_loop(0, CAP // PAIR, close, 0)
    for j in range(1, nt):
        at = ctx.at[pl.ds(0, slices), :]
        remote(at, at, c_send.at[j - 1], c_recv.at[0, j - 1], tensor=(t + j) % nt).wait_send()
    at = wo.at[:, :, pl.ds(0, nb - 1)]
    remote(at, at, d_send.at[0], d_recv.at[0], bal=flip(b, 1)).wait_send()


def encode_all(counts, ordering, tiles, qkv_weight, out_weight):
    nd, nb, nt = (lax.axis_size(name) for name in ("dp", "bal", "tensor"))
    ns = len(bits_of(nb))
    slots, slices, patches = tiles.shape
    kinds, rows, columns = qkv_weight.shape
    width, groups = column_groups(columns)
    waves = len(waves_of(groups))
    lead = pieces_of(slices, QUARTERS)[0][2]
    per = nd // nt
    wq = qkv_weight.reshape(kinds, min(nb, 2), -1, columns)
    wo = out_weight.reshape(nb, -1, columns)
    dtype = tiles.dtype
    vmem = pl.BlockSpec(memory_space=pltpu.VMEM)
    hbm = pl.BlockSpec(memory_space=pltpu.HBM)
    dma = pltpu.SemaphoreType.DMA

    def space(*shape):
        return pltpu.VMEM(shape, dtype)

    buffers = [space(nb >> (s + 1), CAP, slices, patches) for s in range(ns)]
    return pl.pallas_call(
        functools.partial(encode_kernel, (nd, nb, nt)),
        out_shape=jax.ShapeDtypeStruct((CAP, slices, patches), dtype),
        in_specs=[hbm] * 5,
        out_specs=vmem,
        scratch_shapes=buffers
        + buffers
        + [
            space(slots, lead, patches),
            space(slots, slices - lead, patches),
            space(CAP, nt * slices, patches),
            space(kinds, nd, *wq.shape[1:]),
            space(groups, kinds * width, nt * slices),
            space(*wo.shape),
            space(nt, per, *wo.shape),
            space(nt * slices, CAP * patches),
            space(kinds, columns, CAP * patches),
            space(nt * slices, CAP * patches),
            space(per, slices // per, CAP * patches),
        ]
        + [pltpu.SMEM(counts.shape, counts.dtype), pltpu.SMEM(ordering.shape, ordering.dtype)]
        + [
            dma((nb >> (s + 1), len(step_pieces(slices, s == ns - 1))))
            for s in range(ns)
        ]
        + [dma((ns, max(nb // 2, 1))), dma((nt - 1,)), dma((CAP, nt - 1))]
        + [dma((nt - 1,)), dma((CAP // PAIR, nt - 1))]
        + [dma((2, nd - 1, 2)), dma((nd, waves + 1)), dma((1,)), dma((waves,))]
        + [dma((1,)), dma((nt,)), dma((1,)), dma((per,)), dma((max(ns - 1, 1), per)), dma((6,))],
        compiler_params=pltpu.CompilerParams(
            collective_id=0, has_side_effects=True, vmem_limit_bytes=44 * 1024 * 1024
        ),
        name="encode_all",
    )(*(pltpu.with_memory_space_constraint(a, pltpu.HBM) for a in (counts, ordering, tiles, wq, wo)))


def local(tiles, tile_counts, doc_order, qkv_weight, out_weight):
    own_tiles = tiles[0, 0]
    return encode_all(tile_counts, doc_order, own_tiles, qkv_weight, out_weight)[None]


def solution(mesh):
    placed = (
        P("dp", "bal", None, "tensor", None),
        P("dp", None),
        P("dp", None),
        P(None, "dp", "tensor"),
        P("dp", "tensor"),
    )
    return jax.shard_map(
        local, mesh=mesh, in_specs=placed, out_specs=P("dp", "bal", "tensor", None), check_vma=False
    )
```
